32 devices in a mesh: dev: 16 (over z, y, x), rep: 2 (over core).
Axes of the slice: x: 2, y: 2, z: 4, core: 2. Of those that a mesh axis runs over, the one named last changes fastest.
Arguments:
- tables: bfloat16 [64, 2048, 128], P('dev'), may hold values from -1.5 to 1.5
- bag_rows: int32 [32, 64, 32, 4], P(('rep', 'dev')), parts along dimension 0, may hold values from 0 to 2047
- bag_lengths: int32 [32, 64, 32], P(('rep', 'dev')), parts along dimension 0, may hold values from 1 to 4
- row_counts: int32 [32, 64], P(('rep', 'dev')), parts along dimension 0, may hold values from 1 to 32, as said below
- inverse: int32 [4096, 64], P(('rep', 'dev')), parts along dimension 0, may hold values from 0 to 31
- table_order: int32 [64], replicated, may hold values from 0 to 63, each once
- compress: bfloat16 [16, 64], replicated, may hold values from -0.75 to 0.75
- top_weight: bfloat16 [1024, 512], replicated, may hold values from -0.1875 to 0.1875
- top_bias: float32 [512], replicated, may hold values from -1.8 to 1.8
Outputs:
- ranked: bfloat16 [4096, 512], P(('rep', 'dev')), parts along dimension 0
The draws below stay inside these ranges and needn't reach their ends.
There are 2 independent parts, one for each index of `rep`. The reference program is written for one: setup_inputs(seed, part) draws one part's arguments, and reference() takes and returns one part's arrays. A program takes and returns all parts, laid end to end along the dimension named above; an argument that names none is the same for every part. Nothing has to cross between parts.
Inputs may be any that keep to these rules, and one draw needn't show every extreme that they name: `row_counts`: for every sample device and every aligned group of 4 consecutive slots the counts sum to at most 80; a count of 32 and a group sum of 80 occur in every draw.
All inputs are finite; a program needn't handle non-finite values.
Results may differ from the reference program's by a relative error of at most 0.0062.
Values may be sent and summed in bfloat16 or wider, within the bound.
A program may use at most 128 MiB of HBM per device.

```python
import math
import jax
import jax.numpy as jnp
import numpy as np
from jax import lax

WIDTH = 128
VOCABULARY = 2048
TABLES_DEV = 4
TABLES = 64
BATCH_DEV = 128
BATCH = 2048
ROWS_MOST = 32
PACK_ROOM = 80
POOLING = 4
COMPRESSED = 16
TOP_UNITS = 512
N_DEV = 16


def draw_row_counts(key, part):
    first_key = jax.random.fold_in(key, 11)
    second_key = jax.random.fold_in(key, 12)
    third_key = jax.random.fold_in(key, 13)
    raw_counts = jax.random.randint(first_key, (N_DEV, N_DEV, TABLES_DEV), 1, ROWS_MOST + 1)
    group_total = jnp.sum(raw_counts, axis=2, keepdims=True)
    shrunk = 1 + (raw_counts - 1) * (PACK_ROOM - TABLES_DEV) // jnp.maximum(group_total - TABLES_DEV, 1)
    scaled = jnp.where(group_total > PACK_ROOM, shrunk, raw_counts)
    shift_value = jax.random.randint(second_key, (), 0, 5)
    device_range = jnp.arange(N_DEV, dtype=jnp.int32)[:, None]
    group_range = jnp.arange(N_DEV, dtype=jnp.int32)[None, :]
    forced = (device_range * 3 + group_range + shift_value) % 5 == 0
    leader = jax.random.randint(third_key, (N_DEV, N_DEV), 0, TABLES_DEV)
    remainder = PACK_ROOM - ROWS_MOST
    share_value = remainder // (TABLES_DEV - 1)
    last_value = remainder - (TABLES_DEV - 2) * share_value
    member = jnp.arange(TABLES_DEV, dtype=jnp.int32)[None, None, :]
    ranking = (member - leader[..., None]) % TABLES_DEV
    filled = jnp.where(ranking == 0, ROWS_MOST, jnp.where(ranking == TABLES_DEV - 1, last_value, share_value))
    result = jnp.where(forced[..., None], filled, scaled)
    return result.reshape(N_DEV, TABLES).astype(jnp.int32)


def with_ends(values, rng, smallest, largest):
    longest = values.shape.index(max(values.shape))
    spots = []
    for shift in (0, 1):
        where = [jax.random.randint(jax.random.fold_in(rng, axis), (), 0, length) for axis, length in enumerate(values.shape)]
        where[longest] = (where[longest] + shift) % values.shape[longest]
        spots.append(tuple(where))
    return values.at[spots[0]].set(smallest).at[spots[1]].set(largest)


def levels(own_key, dims, cuts, least, top_value):
    factor_of, own = 1.0, jax.random.fold_in(own_key, 6)
    for axis_at, blocks in cuts:
        heights = jnp.exp(jax.random.uniform(jax.random.fold_in(own, axis_at), (blocks,), jnp.float32, least / len(cuts), top_value / len(cuts)))
        factor_of = factor_of * jnp.repeat(heights, dims[axis_at] // blocks).reshape([-1 if axis == axis_at else 1 for axis in range(len(dims))])
    return factor_of


def rank_bounds(count, skew):
    weights = [(1 << 20) // math.isqrt(standing ** skew) + 1 for standing in range(1, count + 1)]
    width = 1 + sum(weights) // (1 << 30)
    return np.cumsum(np.array([max(1, weight // width) for weight in weights]))


def ranked_ids(stream_key, extent, number_of, skew):
    listing = rank_bounds(number_of, skew)
    pick = jax.random.randint(jax.random.fold_in(stream_key, 1), extent, 0, int(listing[number_of - 1]))
    rank = jnp.searchsorted(jnp.asarray(listing, jnp.int32), pick, side="right")
    return jax.random.permutation(jax.random.fold_in(stream_key, 2), number_of)[rank].astype(jnp.int32)


def gaussian(own_key, dims, scale, bound, split=(), kind=jnp.bfloat16):
    drawn = scale * jax.random.normal(own_key, dims, jnp.float32)
    if split:
        drawn = drawn * levels(own_key, dims, split, -0.22, 0.18)
    return jnp.clip(drawn, -bound, bound).astype(kind)


def setup_inputs(seed: int = 0, part: int = 0) -> dict:
    seeds = jax.random.split(jax.random.key(seed), 10)
    part_keys = jax.random.split(jax.random.fold_in(seeds[9], part), 10)
    tables = gaussian(seeds[0], (TABLES, VOCABULARY, WIDTH), 0.25, 1.5, ((0, 16),))
    bag_rows = with_ends(ranked_ids(part_keys[1], (N_DEV, TABLES, ROWS_MOST, POOLING), VOCABULARY, 2), jax.random.fold_in(part_keys[1], 3), 0, VOCABULARY - 1).astype(jnp.int32)
    bag_lengths = with_ends(jax.random.randint(part_keys[2], (N_DEV, TABLES, ROWS_MOST), 1, POOLING + 1), jax.random.fold_in(part_keys[2], 1), 1, POOLING).astype(jnp.int32)
    row_counts = draw_row_counts(jax.random.fold_in(jax.random.fold_in(seeds[9], part), 71), part)
    inverse = with_ends(jax.random.randint(part_keys[4], (BATCH, TABLES), 0, ROWS_MOST), jax.random.fold_in(part_keys[4], 1), 0, ROWS_MOST - 1).astype(jnp.int32)
    table_order = jax.random.permutation(seeds[5], TABLES).astype(jnp.int32)
    compress = gaussian(seeds[6], (COMPRESSED, TABLES), TABLES ** -0.5, 0.75)
    top_weight = gaussian(seeds[7], (TABLES * COMPRESSED, TOP_UNITS), (TABLES * COMPRESSED) ** -0.5, 0.1875)
    top_bias = gaussian(seeds[8], (TOP_UNITS,), 0.3, 1.8, (), jnp.float32)
    return {"tables": tables, "bag_rows": bag_rows, "bag_lengths": bag_lengths, "row_counts": row_counts, "inverse": inverse, "table_order": table_order, "compress": compress, "top_weight": top_weight, "top_bias": top_bias}


def pool_rows(tables, rows_here, lengths_here):
    gathered = jax.vmap(lambda one_table, one_bag: jnp.take(one_table, one_bag, axis=0))(tables, rows_here)
    active = jnp.arange(rows_here.shape[2], dtype=jnp.int32)[None, None, :] < lengths_here[..., None]
    summed = jnp.sum(jnp.where(active[..., None], gathered.astype(jnp.float32), jnp.zeros((), jnp.float32)), axis=2)
    return summed.astype(jnp.bfloat16)


def interact(features, compress, top_weight, top_bias):
    mixed = jnp.einsum("kf,bfe->bke", compress.astype(jnp.float32), features.astype(jnp.float32)).astype(jnp.bfloat16)
    pairwise = jnp.einsum("bfe,bke->bfk", features.astype(jnp.float32), mixed.astype(jnp.float32)).astype(jnp.bfloat16)
    hidden_pre = jnp.dot(pairwise.reshape(pairwise.shape[0], -1), top_weight, preferred_element_type=jnp.float32) + top_bias
    return jnp.maximum(hidden_pre, jnp.zeros((), jnp.float32)).astype(jnp.bfloat16)


def reference(tables, bag_rows, bag_lengths, row_counts, inverse, table_order, compress, top_weight, top_bias):
    slot_range = jnp.arange(TABLES, dtype=jnp.int32)
    matches = table_order[:, None] == slot_range[None, :]
    slot_of = jnp.sum(jnp.where(matches, slot_range[:, None], 0), axis=0).astype(jnp.int32)

    def one_device(device):
        rows_here = lax.dynamic_index_in_dim(bag_rows, device, 0, keepdims=False)
        lengths_here = lax.dynamic_index_in_dim(bag_lengths, device, 0, keepdims=False)
        counts_here = lax.dynamic_index_in_dim(row_counts, device, 0, keepdims=False)
        inverse_here = lax.dynamic_slice_in_dim(inverse, (device * BATCH_DEV).astype(jnp.int32), BATCH_DEV, 0)
        pooled = pool_rows(tables, rows_here, lengths_here)
        flat_rows = pooled.reshape(-1, WIDTH)
        positions = (slot_of[None, :] * ROWS_MOST + inverse_here).astype(jnp.int32)
        gathered = jnp.take(flat_rows, positions, axis=0)
        present = inverse_here < counts_here[slot_of][None, :]
        features = jnp.where(present[..., None], gathered, jnp.zeros((), jnp.bfloat16))
        return interact(features, compress, top_weight, top_bias)

    result = lax.map(one_device, jnp.arange(N_DEV, dtype=jnp.int32))
    return result.reshape(BATCH, TOP_UNITS)
```

```python
import functools

import jax
import jax.numpy as jnp
from jax import lax
from jax.experimental import pallas as pl
from jax.experimental.pallas import tpu as pltpu
from jax.sharding import PartitionSpec as P

F32 = jnp.float32
BF16 = jnp.bfloat16
I32 = jnp.int32
LANES = 128
PACK_GROUP, PACK_ROOM = 4, 80


def iota(shape, axis):
    return lax.broadcasted_iota(I32, shape, axis)


def flip(me, m, n):
    out, bit = me, 1
    while bit < n:
        out = out + ((m // bit) % 2) * (1 - 2 * ((me // bit) % 2)) * bit
        bit *= 2
    return out


def loop(start, stop, body, unroll=False):
    def step(i, carry):
        body(i)
        return carry

    lax.fori_loop(start, stop, step, 0, unroll=unroll)


def pack_ids(q, most, vocab, zero_row, counts, xt, lt, ids_out):
    pooling = ids_out.shape[1]
    tabs = PACK_GROUP
    shape = (2 * pooling, LANES)
    sub, lane = iota(shape, 0), iota(shape, 1)
    high, p = sub >= pooling, sub % pooling
    first, second = 2 * q * tabs, (2 * q + 1) * tabs
    off_a, off_b = jnp.int32(0), jnp.int32(0)
    ids = jnp.full(shape, zero_row, I32)
    for t in range(tabs):
        count_a, count_b = counts[first + t], counts[second + t]
        unit = lane - jnp.where(high, off_b, off_a)
        at = jnp.clip(unit, 0, most - 1)
        rows = jnp.where(high, xt[pl.ds(second + t, 1), :], xt[pl.ds(first + t, 1), :])
        lengths = jnp.where(high, lt[pl.ds(second + t, 1), :], lt[pl.ds(first + t, 1), :])
        row = jnp.take_along_axis(rows, at * pooling + p, axis=1, mode="promise_in_bounds")
        length = jnp.take_along_axis(lengths, at, axis=1, mode="promise_in_bounds")
        used = (unit >= 0) & (unit < jnp.where(high, count_b, count_a)) & (p < length)
        ids = jnp.where(used, row + t * vocab, ids)
        off_a, off_b = off_a + count_a, off_b + count_b
    ids_out[2 * q] = ids[:pooling]
    ids_out[2 * q + 1] = ids[pooling:]


def place_targets(g, order, counts, inv, targets, expand):
    tabs = PACK_GROUP
    feature = iota((1, expand.shape[1]), 1)
    off = jnp.int32(0)
    for t in range(tabs):
        s = g * tabs + t
        count = counts[s]
        row = inv[pl.ds(order[s], 1), :]
        row = jnp.where(row < count, row + off, -1)
        targets[g, t:t + 1, :] = row
        targets[g, tabs + t:tabs + t + 1, :] = pltpu.roll(row, row.shape[1] - 4, 1)
        off = off + count
        hot = jnp.where(feature == order[s], 1.0, 0.0)
        expand[pl.ds(g * 2 * tabs + t, 1), :] = hot
        expand[pl.ds(g * 2 * tabs + tabs + t, 1), :] = hot


def choose_rows(target, choice, at):
    samples = target.shape[1]
    lane = iota((16, LANES), 1)
    pairs = [blk * 8 + b for blk in range(samples // 8) for b in range(4)]
    for i in range(0, len(pairs), 2):
        wide = jnp.concatenate(
            [jnp.broadcast_to(target[:, c:c + 1], (8, LANES)) for c in pairs[i:i + 2]], axis=0
        )
        choice[at, i * 8:i * 8 + 16, :] = jnp.where(wide == lane, 1.0, 0.0).astype(BF16)


def exchange_kernel(
    n, most, room,
    bags_hbm, lens_hbm, tables_hbm, inv_hbm, order_hbm, counts_hbm, compress_hbm, weight_hbm,
    f_ref, mixer_ref, w_ref,
    bags, lens, tab16, inv, order, counts, compress, weight,
    tab32, xt, lt, ids_out, ids_in, pooled, staging, rows, targets, expand, choice,
    local, own_sem, id_send, id_recv, row_send, row_recv,
):
    me = lax.axis_index("dev")
    tabs, vocab, width = tab16.shape
    slots, samples = inv.shape
    mixes = compress.shape[0]
    pooling = ids_out.shape[1]
    zero_row = tabs * vocab
    small = n <= 16

    barrier = pltpu.get_barrier_semaphore()
    loop(1, n, lambda m: pl.semaphore_signal(barrier, inc=1, device_id={"dev": flip(me, m, n)}))

    copies = [
        pltpu.make_async_copy(src, dst, local.at[i])
        for i, (src, dst) in enumerate([
            (counts_hbm, counts), (bags_hbm, bags), (lens_hbm, lens), (order_hbm, order),
            (inv_hbm, inv), (compress_hbm, compress), (tables_hbm, tab16), (weight_hbm, weight),
        ])
    ]
    for copy in copies:
        copy.start()
    counts_in, bags_in, lens_in, order_in, inv_in, compress_in, tables_in, weight_in = copies

    bags_in.wait()
    xt[...] = bags[...].T
    lens_in.wait()
    lt[...] = jnp.concatenate(
        [lens[...], jnp.zeros((LANES - most, slots), I32)], axis=0
    ).T
    counts_in.wait()
    loop(
        0, n // 2, lambda q: pack_ids(q, most, vocab, zero_row, counts, xt, lt, ids_out),
        unroll=small,
    )
    pl.semaphore_wait(barrier, n - 1)

    def id_copy(m):
        peer = flip(me, m, n)
        return pltpu.make_async_remote_copy(
            src_ref=ids_out.at[peer], dst_ref=ids_in.at[m],
            send_sem=id_send.at[m], recv_sem=id_recv.at[m],
            device_id={"dev": peer},
        )

    def row_copy(m):
        peer = flip(me, m, n)
        return pltpu.make_async_remote_copy(
            src_ref=staging.at[m], dst_ref=rows.at[me],
            send_sem=row_send.at[m], recv_sem=row_recv.at[me],
            device_id={"dev": peer},
        )

    loop(1, n, lambda m: id_copy(m).start())
    own_ids = pltpu.make_async_copy(ids_out.at[me], ids_in.at[0], own_sem)
    own_ids.start()

    tables_in.wait()
    tab32[pl.ds(zero_row, 8), :] = jnp.zeros((8, width), F32)
    step = 256

    def widen(i):
        for t in range(tabs):
            base = pl.multiple_of(i * step, step)
            tab32[pl.ds(t * vocab + base, step), :] = tab16[t, pl.ds(base, step), :].astype(F32)

    loop(0, vocab // step, widen)

    order_in.wait()
    inv_in.wait()
    loop(0, n, lambda g: place_targets(g, order, counts, inv, targets, expand))
    if small:
        loop(0, n, lambda g: choose_rows(targets[g], choice, g))

    weight_in.wait()
    group = 8
    inner = group * mixes
    r, c = iota((inner, inner), 0), iota((inner, inner), 1)
    source = ((r // 8) % 2 * tabs + r % tabs) * mixes + 2 * (r // 16) + (r // 4) % 2
    reorder = jnp.where(c == source, 1.0, 0.0).astype(BF16)

    def order_weight(q):
        block = jnp.concatenate([weight[order[q * group + i]] for i in range(group)], axis=0)
        moved = jnp.dot(reorder, block, preferred_element_type=F32).astype(BF16)
        w_ref[:, pl.ds(pl.multiple_of(q * 16, 16), 16), :] = moved.reshape(mixes // 2, 16, -1)

    loop(0, slots // group, order_weight)

    compress_in.wait()
    across = f_ref.shape[1]
    spread = lax.dot_general(
        compress[...], expand[...].astype(BF16), (((1,), (1,)), ((), ())),
        preferred_element_type=F32,
    )
    sub, lane = iota((8, across), 0), iota((8, across), 1)
    same_half = (lane // tabs) % 2 == sub // 4
    for k in range(0, mixes, 2):
        for b in range(4):
            held = same_half & (sub % 4 == b)
            kept = [
                jnp.where(held, jnp.broadcast_to(spread[k + h:k + h + 1, :], (8, across)), 0.0)
                for h in range(2)
            ]
            mixer_ref[k * 8:k * 8 + 16, b * across:(b + 1) * across] = (
                jnp.concatenate(kept, axis=0).astype(BF16)
            )

    def pool(m, store):
        def row_block(i):
            at = pl.multiple_of(i * 16, 16)
            for r in range(16):
                total = None
                for p in range(pooling):
                    row = tab32[pl.ds(ids_in[m, p, at + r], 1), :]
                    total = row if total is None else total + row
                pooled[pl.ds(at + r, 1), :] = total

        loop(0, room // 16, row_block, unroll=True)
        store(pooled[...].astype(BF16))

    own_ids.wait()

    def store_own(value):
        rows[me] = value

    pool(0, store_own)

    def serve(m):
        id_copy(m).wait_recv()

        def store(value):
            staging[m] = value

        pool(m, store)
        row_copy(m).start()

    loop(1, n, serve)

    def select(i):
        q = flip(me // 2, i, n // 2)
        features = []
        for h in range(2):
            g = 2 * q + h
            at = g
            if not small:
                at = h
                choose_rows(targets[g], choice, h)
            packed = jnp.concatenate([rows[g], jnp.zeros((LANES - room, width), BF16)], axis=0)
            chosen = jnp.dot(choice[at], packed, preferred_element_type=F32)
            features.append(chosen.reshape(samples // 2, 8, width))
        f_ref[:, pl.ds(pl.multiple_of(q * 16, 16), 16), :] = (
            jnp.concatenate(features, axis=1).astype(BF16)
        )

    def arrival(m):
        peer = flip(me, m, n)
        pltpu.make_async_remote_copy(
            src_ref=staging.at[m], dst_ref=rows.at[peer],
            send_sem=row_send.at[m], recv_sem=row_recv.at[peer],
            device_id={"dev": peer},
        ).wait_recv()

    arrival(1)
    select(0)

    def collect(i):
        arrival(2 * i)
        arrival(2 * i + 1)
        select(i)

    loop(1, n // 2, collect)

    def finish(m):
        id_copy(m).wait_send()
        row_copy(m).wait_send()

    loop(1, n, finish)


def exchange(n, bags, lens, tables, inv, order, counts, compress, weight):
    tabs, vocab, width = tables.shape
    rows, slots = bags.shape
    most = lens.shape[0]
    pooling = rows // most
    samples, mixes, units = inv.shape[1], compress.shape[0], weight.shape[-1]
    room = PACK_ROOM
    assert tabs == PACK_GROUP and pooling == 4 and rows == LANES and n & (n - 1) == 0
    across = 2 * slots
    held = 3 * tables.size * 2 + 3 * weight.size * 2 + 3 * n * room * width * 4
    held += (samples * across * width + min(n, 16) * 4 * samples * LANES) * 2
    in_hbm = pl.BlockSpec(memory_space=pltpu.HBM)
    vmem = pl.BlockSpec(memory_space=pltpu.VMEM)
    operands = [
        pltpu.with_memory_space_constraint(x, pltpu.HBM)
        for x in (bags, lens, tables, inv, order, counts, compress, weight)
    ]
    return pl.pallas_call(
        functools.partial(exchange_kernel, n, most, room),
        out_shape=[
            jax.ShapeDtypeStruct((samples // 2, across, width), BF16),
            jax.ShapeDtypeStruct((mixes * 8, 4 * across), BF16),
            jax.ShapeDtypeStruct((mixes // 2, across, units), BF16),
        ],
        in_specs=[in_hbm] * 8,
        out_specs=[vmem] * 3,
        scratch_shapes=[
            pltpu.VMEM(bags.shape, I32),
            pltpu.VMEM(lens.shape, I32),
            pltpu.VMEM(tables.shape, BF16),
            pltpu.VMEM(inv.shape, I32),
            pltpu.SMEM(order.shape, I32),
            pltpu.SMEM(counts.shape, I32),
            pltpu.VMEM(compress.shape, BF16),
            pltpu.VMEM(weight.shape, BF16),
            pltpu.VMEM((tabs * vocab + 8, width), F32),
            pltpu.VMEM((slots, LANES), I32),
            pltpu.VMEM((slots, LANES), I32),
            pltpu.VMEM((n, pooling, LANES), I32),
            pltpu.SMEM((n, pooling, LANES), I32),
            pltpu.VMEM((room, width), F32),
            pltpu.VMEM((n, room, width), BF16),
            pltpu.VMEM((n, room, width), BF16),
            pltpu.VMEM((n, 2 * tabs, samples), I32),
            pltpu.VMEM((across, slots), F32),
            pltpu.VMEM((n if n <= 16 else 2, 4 * samples, LANES), BF16),
            pltpu.SemaphoreType.DMA((8,)),
            pltpu.SemaphoreType.DMA,
            pltpu.SemaphoreType.DMA((n,)),
            pltpu.SemaphoreType.DMA((n,)),
            pltpu.SemaphoreType.DMA((n,)),
            pltpu.SemaphoreType.DMA((n,)),
        ],
        compiler_params=pltpu.CompilerParams(
            collective_id=0, has_side_effects=True, vmem_limit_bytes=min(63 << 20, held + (6 << 20))
        ),
        name="exchange",
    )(*operands)


def interact_kernel(f_ref, mixer_ref, w_ref, bias_ref, out_ref, pairs):
    across, width = f_ref.shape[1:]
    mixes = mixer_ref.shape[0] // 8
    samples = out_ref.shape[0]
    sub, lane = iota((8, across), 0), iota((8, across), 1)
    first = sub < 4
    in_place = (lane // 4) % 2 == sub // 4
    mine = [sub % 4 == b for b in range(4)]

    def block(j):
        features = f_ref[pl.ds(j * 4, 4)].reshape(4 * across, width)
        mixed = jnp.dot(mixer_ref[...], features, preferred_element_type=F32).astype(BF16)
        products = lax.dot_general(
            mixed, features, (((1,), (1,)), ((), ())), preferred_element_type=F32
        )

        def of_mixture(k):
            parts = products[k * 8:k * 8 + 8, :]
            out = parts[:, :across]
            for b in range(1, 4):
                out = jnp.where(mine[b], parts[:, b * across:(b + 1) * across], out)
            return out

        for k in range(0, mixes, 2):
            even, odd = of_mixture(k), of_mixture(k + 1)
            stay, move = jnp.where(first, even, odd), jnp.where(first, odd, even)
            moved = jnp.where(first, pltpu.roll(move, 4, 1), pltpu.roll(move, across - 4, 1))
            pairs[pl.ds(pl.multiple_of(j * 8, 8), 8), k // 2 * across:(k // 2 + 1) * across] = (
                jnp.where(in_place, stay, moved)
            )

    loop(0, samples // 8, block)
    hidden = jnp.dot(
        pairs[...].astype(BF16), w_ref[...].reshape(mixes // 2 * across, -1),
        preferred_element_type=F32,
    ) + bias_ref[...]
    out_ref[...] = jnp.maximum(hidden, 0.0).astype(BF16)


def interact(features, mixer, weight, bias):
    pairs_of_samples, across, _ = features.shape
    samples, half_mixes, units = 2 * pairs_of_samples, weight.shape[0], weight.shape[2]
    held = (features.size + 2 * weight.size + mixer.size) * 2 + 6 * samples * half_mixes * across
    vmem = pl.BlockSpec(memory_space=pltpu.VMEM)
    return pl.pallas_call(
        interact_kernel,
        out_shape=jax.ShapeDtypeStruct((samples, units), BF16),
        in_specs=[vmem] * 4,
        out_specs=vmem,
        scratch_shapes=[pltpu.VMEM((samples, half_mixes * across), F32)],
        compiler_params=pltpu.CompilerParams(vmem_limit_bytes=min(63 << 20, held + (6 << 20))),
        name="interact",
    )(features, mixer, weight, bias)


def shards(
    n, tables, bag_rows, bag_lengths, row_counts, inverse, table_order, compress, top_weight, top_bias
):
    _, slots, most, pooling = bag_rows.shape
    mixes = compress.shape[0]
    features, mixer, weight = exchange(
        n, bag_rows[0].transpose(1, 2, 0).reshape(most * pooling, slots), bag_lengths[0].T, tables,
        inverse.T, table_order, row_counts[0], compress, top_weight.reshape(slots, mixes, -1),
    )
    return interact(features, mixer, weight, top_bias.reshape(1, -1))


def solution(mesh):
    return jax.shard_map(
        functools.partial(shards, mesh.shape["dev"]),
        mesh=mesh,
        in_specs=(
            P("dev", None, None),
            P(("rep", "dev"), None, None, None),
            P(("rep", "dev"), None, None),
            P(("rep", "dev"), None),
            P(("rep", "dev"), None),
            P(),
            P(),
            P(),
            P(),
        ),
        out_specs=P(("rep", "dev"), None),
        check_vma=False,
    )
```

```python
import functools

import jax
import jax.numpy as jnp
from jax import lax
from jax.experimental import pallas as pl
from jax.experimental.pallas import tpu as pltpu
from jax.sharding import PartitionSpec as P

F32 = jnp.float32
BF16 = jnp.bfloat16
I32 = jnp.int32
LANES = 128
PACK_GROUP, PACK_ROOM = 4, 80


def iota(shape, axis):
    return lax.broadcasted_iota(I32, shape, axis)


def flip(me, m, n):
    out, bit = me, 1
    while bit < n:
        if not isinstance(m, int):
            out = out + ((m // bit) % 2) * (1 - 2 * ((me // bit) % 2)) * bit
        elif m // bit % 2:
            out = out + (bit - 2 * bit * ((me // bit) % 2))
        bit *= 2
    return out


def loop(start, stop, body, unroll=False):
    if unroll is True and stop - start <= 16:
        for i in range(start, stop):
            body(i)
        return

    def step(i, carry):
        body(i)
        return carry

    lax.fori_loop(start, stop, step, 0, unroll=unroll)


def pack_ids(q, most, vocab, zero_row, counts, xt, lt, ids_out):
    pooling = ids_out.shape[1]
    tabs = PACK_GROUP
    shape = (2 * pooling, LANES)
    sub, lane = iota(shape, 0), iota(shape, 1)
    high, p = sub >= pooling, sub % pooling
    first, second = 2 * q * tabs, (2 * q + 1) * tabs
    off_a, off_b = jnp.int32(0), jnp.int32(0)
    ids = jnp.full(shape, zero_row, I32)
    for t in range(tabs):
        count_a, count_b = counts[first + t], counts[second + t]
        unit = lane - jnp.where(high, off_b, off_a)
        at = jnp.clip(unit, 0, most - 1)
        rows = jnp.where(high, xt[pl.ds(second + t, 1), :], xt[pl.ds(first + t, 1), :])
        lengths = jnp.where(high, lt[pl.ds(second + t, 1), :], lt[pl.ds(first + t, 1), :])
        row = jnp.take_along_axis(rows, at * pooling + p, axis=1, mode="promise_in_bounds")
        length = jnp.take_along_axis(lengths, at, axis=1, mode="promise_in_bounds")
        used = (unit >= 0) & (unit < jnp.where(high, count_b, count_a)) & (p < length)
        ids = jnp.where(used, row + t * vocab, ids)
        off_a, off_b = off_a + count_a, off_b + count_b
    ids_out[2 * q] = ids[:pooling]
    ids_out[2 * q + 1] = ids[pooling:]


def place_targets(g, order, counts, inv, targets, expand):
    tabs = PACK_GROUP
    feature = iota((1, expand.shape[1]), 1)
    off = jnp.int32(0)
    for t in range(tabs):
        s = g * tabs + t
        count = counts[s]
        row = inv[pl.ds(order[s], 1), :]
        row = jnp.where(row < count, row + off, -1)
        targets[g, t:t + 1, :] = row
        targets[g, tabs + t:tabs + t + 1, :] = pltpu.roll(row, row.shape[1] - 4, 1)
        off = off + count
        hot = jnp.where(feature == order[s], 1.0, 0.0)
        expand[pl.ds(g * 2 * tabs + t, 1), :] = hot
        expand[pl.ds(g * 2 * tabs + tabs + t, 1), :] = hot


def choose_rows(target, choice, at):
    samples = target.shape[1]
    lane = iota((16, LANES), 1)
    pairs = [blk * 8 + b for blk in range(samples // 8) for b in range(4)]
    for i in range(0, len(pairs), 2):
        wide = jnp.concatenate(
            [jnp.broadcast_to(target[:, c:c + 1], (8, LANES)) for c in pairs[i:i + 2]], axis=0
        )
        choice[at, i * 8:i * 8 + 16, :] = jnp.where(wide == lane, 1.0, 0.0).astype(BF16)


def exchange_kernel(
    n, most, room,
    bags_hbm, lens_hbm, tables_hbm, inv_hbm, order_hbm, counts_hbm, compress_hbm, weight_hbm,
    f_ref, mixer_ref, w_ref,
    bags, lens, tab16, inv, order, counts, compress, weight,
    tab32, xt, lt, ids_out, ids_in, pooled, staging, rows, targets, expand, choice,
    local, own_sem, id_send, id_recv, row_send, row_recv,
):
    me = lax.axis_index("dev")
    tabs, vocab, width = tab16.shape
    slots, samples = inv.shape
    mixes = compress.shape[0]
    pooling = ids_out.shape[1]
    zero_row = tabs * vocab
    small = n <= 16

    barrier = pltpu.get_barrier_semaphore()
    loop(
        1, n,
        lambda m: pl.semaphore_signal(barrier, inc=1, device_id={"dev": flip(me, m, n)}),
        unroll=small,
    )

    copies = [
        pltpu.make_async_copy(src, dst, local.at[i])
        for i, (src, dst) in enumerate([
            (counts_hbm, counts), (bags_hbm, bags), (lens_hbm, lens), (order_hbm, order),
            (inv_hbm, inv), (compress_hbm, compress), (tables_hbm, tab16), (weight_hbm, weight),
        ])
    ]
    for copy in copies:
        copy.start()
    counts_in, bags_in, lens_in, order_in, inv_in, compress_in, tables_in, weight_in = copies

    bags_in.wait()
    xt[...] = bags[...].T
    lens_in.wait()
    lt[...] = jnp.concatenate(
        [lens[...], jnp.zeros((LANES - most, slots), I32)], axis=0
    ).T
    counts_in.wait()
    loop(
        0, n // 2, lambda q: pack_ids(q, most, vocab, zero_row, counts, xt, lt, ids_out),
        unroll=small,
    )
    order_in.wait()
    inv_in.wait()
    loop(0, n, lambda g: place_targets(g, order, counts, inv, targets, expand), unroll=4)
    if small:
        loop(0, n, lambda g: choose_rows(targets[g], choice, g), unroll=4)

    pl.semaphore_wait(barrier, n - 1)

    def id_copy(m):
        peer = flip(me, m, n)
        return pltpu.make_async_remote_copy(
            src_ref=ids_out.at[peer], dst_ref=ids_in.at[m],
            send_sem=id_send.at[m], recv_sem=id_recv.at[m],
            device_id={"dev": peer},
        )

    def row_copy(m):
        peer = flip(me, m, n)
        return pltpu.make_async_remote_copy(
            src_ref=staging.at[m], dst_ref=rows.at[me],
            send_sem=row_send.at[m], recv_sem=row_recv.at[me],
            device_id={"dev": peer},
        )

    loop(1, n, lambda m: id_copy(m).start(), unroll=small)
    own_ids = pltpu.make_async_copy(ids_out.at[me], ids_in.at[0], own_sem)
    own_ids.start()

    tables_in.wait()
    tab32[pl.ds(zero_row, 8), :] = jnp.zeros((8, width), F32)
    step = 256

    def widen(i):
        for t in range(tabs):
            base = pl.multiple_of(i * step, step)
            tab32[pl.ds(t * vocab + base, step), :] = tab16[t, pl.ds(base, step), :].astype(F32)

    loop(0, vocab // step, widen)

    weight_in.wait()
    group = 8
    inner = group * mixes
    r, c = iota((inner, inner), 0), iota((inner, inner), 1)
    source = ((r // 8) % 2 * tabs + r % tabs) * mixes + 2 * (r // 16) + (r // 4) % 2
    reorder = jnp.where(c == source, 1.0, 0.0).astype(BF16)

    def order_weight(q):
        block = jnp.concatenate([weight[order[q * group + i]] for i in range(group)], axis=0)
        moved = jnp.dot(reorder, block, preferred_element_type=F32).astype(BF16)
        w_ref[:, pl.ds(pl.multiple_of(q * 16, 16), 16), :] = moved.reshape(mixes // 2, 16, -1)

    loop(0, slots // group, order_weight, unroll=4)

    compress_in.wait()
    across = f_ref.shape[1]
    spread = lax.dot_general(
        compress[...], expand[...].astype(BF16), (((1,), (1,)), ((), ())),
        preferred_element_type=F32,
    )
    sub, lane = iota((8, across), 0), iota((8, across), 1)
    same_half = (lane // tabs) % 2 == sub // 4
    for k in range(0, mixes, 2):
        for b in range(4):
            held = same_half & (sub % 4 == b)
            kept = [
                jnp.where(held, jnp.broadcast_to(spread[k + h:k + h + 1, :], (8, across)), 0.0)
                for h in range(2)
            ]
            mixer_ref[k * 8:k * 8 + 16, b * across:(b + 1) * across] = (
                jnp.concatenate(kept, axis=0).astype(BF16)
            )

    def pool(m, store):
        def row_block(i):
            at = pl.multiple_of(i * 16, 16)
            for r in range(16):
                total = None
                for p in range(pooling):
                    row = tab32[pl.ds(ids_in[m, p, at + r], 1), :]
                    total = row if total is None else total + row
                pooled[pl.ds(at + r, 1), :] = total

        loop(0, room // 16, row_block, unroll=True)
        store(pooled[...].astype(BF16))

    own_ids.wait()

    def store_own(value):
        rows[me] = value

    pool(0, store_own)

    def serve(m):
        id_copy(m).wait_recv()

        def store(value):
            staging[m] = value

        pool(m, store)
        row_copy(m).start()

    lax.fori_loop(1, n, lambda i, c: (serve(i), c)[1], 0, unroll=small)

    def select(i):
        q = flip(me // 2, i, n // 2)
        features = []
        for h in range(2):
            g = 2 * q + h
            at = g
            if not small:
                at = h
                choose_rows(targets[g], choice, h)
            packed = jnp.concatenate([rows[g], jnp.zeros((LANES - room, width), BF16)], axis=0)
            chosen = jnp.dot(choice[at], packed, preferred_element_type=F32)
            features.append(chosen.reshape(samples // 2, 8, width))
        f_ref[:, pl.ds(pl.multiple_of(q * 16, 16), 16), :] = (
            jnp.concatenate(features, axis=1).astype(BF16)
        )

    def arrival(m):
        peer = flip(me, m, n)
        pltpu.make_async_remote_copy(
            src_ref=staging.at[m], dst_ref=rows.at[peer],
            send_sem=row_send.at[m], recv_sem=row_recv.at[peer],
            device_id={"dev": peer},
        ).wait_recv()

    arrival(1)
    select(0)

    def collect(i):
        arrival(2 * i)
        arrival(2 * i + 1)
        select(i)

    loop(1, n // 2, collect)

    def finish(m):
        id_copy(m).wait_send()
        row_copy(m).wait_send()

    loop(1, n, finish, unroll=small)


def exchange(n, bags, lens, tables, inv, order, counts, compress, weight):
    tabs, vocab, width = tables.shape
    rows, slots = bags.shape
    most = lens.shape[0]
    pooling = rows // most
    samples, mixes, units = inv.shape[1], compress.shape[0], weight.shape[-1]
    room = PACK_ROOM
    assert tabs == PACK_GROUP and pooling == 4 and rows == LANES and n & (n - 1) == 0
    across = 2 * slots
    held = 3 * tables.size * 2 + 3 * weight.size * 2 + 3 * n * room * width * 4
    held += (samples * across * width + min(n, 16) * 4 * samples * LANES) * 2
    in_hbm = pl.BlockSpec(memory_space=pltpu.HBM)
    vmem = pl.BlockSpec(memory_space=pltpu.VMEM)
    operands = [
        pltpu.with_memory_space_constraint(x, pltpu.HBM)
        for x in (bags, lens, tables, inv, order, counts, compress, weight)
    ]
    return pl.pallas_call(
        functools.partial(exchange_kernel, n, most, room),
        out_shape=[
            jax.ShapeDtypeStruct((samples // 2, across, width), BF16),
            jax.ShapeDtypeStruct((mixes * 8, 4 * across), BF16),
            jax.ShapeDtypeStruct((mixes // 2, across, units), BF16),
        ],
        in_specs=[in_hbm] * 8,
        out_specs=[vmem] * 3,
        scratch_shapes=[
            pltpu.VMEM(bags.shape, I32),
            pltpu.VMEM(lens.shape, I32),
            pltpu.VMEM(tables.shape, BF16),
            pltpu.VMEM(inv.shape, I32),
            pltpu.SMEM(order.shape, I32),
            pltpu.SMEM(counts.shape, I32),
            pltpu.VMEM(compress.shape, BF16),
            pltpu.VMEM(weight.shape, BF16),
            pltpu.VMEM((tabs * vocab + 8, width), F32),
            pltpu.VMEM((slots, LANES), I32),
            pltpu.VMEM((slots, LANES), I32),
            pltpu.VMEM((n, pooling, LANES), I32),
            pltpu.SMEM((n, pooling, LANES), I32),
            pltpu.VMEM((room, width), F32),
            pltpu.VMEM((n, room, width), BF16),
            pltpu.VMEM((n, room, width), BF16),
            pltpu.VMEM((n, 2 * tabs, samples), I32),
            pltpu.VMEM((across, slots), F32),
            pltpu.VMEM((n if n <= 16 else 2, 4 * samples, LANES), BF16),
            pltpu.SemaphoreType.DMA((8,)),
            pltpu.SemaphoreType.DMA,
            pltpu.SemaphoreType.DMA((n,)),
            pltpu.SemaphoreType.DMA((n,)),
            pltpu.SemaphoreType.DMA((n,)),
            pltpu.SemaphoreType.DMA((n,)),
        ],
        compiler_params=pltpu.CompilerParams(
            collective_id=0, has_side_effects=True, vmem_limit_bytes=min(63 << 20, held + (6 << 20))
        ),
        name="exchange",
    )(*operands)


def interact_kernel(f_ref, mixer_ref, w_ref, bias_ref, out_ref, pairs):
    across, width = f_ref.shape[1:]
    mixes = mixer_ref.shape[0] // 8
    samples = out_ref.shape[0]
    sub, lane = iota((8, across), 0), iota((8, across), 1)
    first = sub < 4
    in_place = (lane // 4) % 2 == sub // 4
    mine = [sub % 4 == b for b in range(4)]

    def block(j):
        features = f_ref[pl.ds(j * 4, 4)].reshape(4 * across, width)
        mixed = jnp.dot(mixer_ref[...], features, preferred_element_type=F32).astype(BF16)
        products = lax.dot_general(
            mixed, features, (((1,), (1,)), ((), ())), preferred_element_type=F32
        )

        def of_mixture(k):
            parts = products[k * 8:k * 8 + 8, :]
            out = parts[:, :across]
            for b in range(1, 4):
                out = jnp.where(mine[b], parts[:, b * across:(b + 1) * across], out)
            return out

        for k in range(0, mixes, 2):
            even, odd = of_mixture(k), of_mixture(k + 1)
            stay, move = jnp.where(first, even, odd), jnp.where(first, odd, even)
            moved = jnp.where(first, pltpu.roll(move, 4, 1), pltpu.roll(move, across - 4, 1))
            pairs[pl.ds(pl.multiple_of(j * 8, 8), 8), k // 2 * across:(k // 2 + 1) * across] = (
                jnp.where(in_place, stay, moved)
            )

    loop(0, samples // 8, block, unroll=samples <= LANES and across <= LANES)
    hidden = jnp.dot(
        pairs[...].astype(BF16), w_ref[...].reshape(mixes // 2 * across, -1),
        preferred_element_type=F32,
    ) + bias_ref[...]
    out_ref[...] = jnp.maximum(hidden, 0.0).astype(BF16)


def interact(features, mixer, weight, bias):
    pairs_of_samples, across, _ = features.shape
    samples, half_mixes, units = 2 * pairs_of_samples, weight.shape[0], weight.shape[2]
    held = (features.size + 2 * weight.size + mixer.size) * 2 + 6 * samples * half_mixes * across
    vmem = pl.BlockSpec(memory_space=pltpu.VMEM)
    return pl.pallas_call(
        interact_kernel,
        out_shape=jax.ShapeDtypeStruct((samples, units), BF16),
        in_specs=[vmem] * 4,
        out_specs=vmem,
        scratch_shapes=[pltpu.VMEM((samples, half_mixes * across), F32)],
        compiler_params=pltpu.CompilerParams(vmem_limit_bytes=min(63 << 20, held + (6 << 20))),
        name="interact",
    )(features, mixer, weight, bias)


def shards(
    n, tables, bag_rows, bag_lengths, row_counts, inverse, table_order, compress, top_weight, top_bias
):
    _, slots, most, pooling = bag_rows.shape
    mixes = compress.shape[0]
    features, mixer, weight = exchange(
        n, bag_rows[0].transpose(1, 2, 0).reshape(most * pooling, slots), bag_lengths[0].T, tables,
        inverse.T, table_order, row_counts[0], compress, top_weight.reshape(slots, mixes, -1),
    )
    return interact(features, mixer, weight, top_bias.reshape(1, -1))


def solution(mesh):
    return jax.shard_map(
        functools.partial(shards, mesh.shape["dev"]),
        mesh=mesh,
        in_specs=(
            P("dev", None, None),
            P(("rep", "dev"), None, None, None),
            P(("rep", "dev"), None, None),
            P(("rep", "dev"), None),
            P(("rep", "dev"), None),
            P(),
            P(),
            P(),
            P(),
        ),
        out_specs=P(("rep", "dev"), None),
        check_vma=False,
    )
```

```python
import functools

import jax
import jax.numpy as jnp
from jax import lax
from jax.experimental import pallas as pl
from jax.experimental.pallas import tpu as pltpu
from jax.sharding import PartitionSpec as P

F32 = jnp.float32
BF16 = jnp.bfloat16
I32 = jnp.int32
LANES = 128
PACK_GROUP, PACK_ROOM = 4, 80


def iota(shape, axis):
    return lax.broadcasted_iota(I32, shape, axis)


def flip(me, m, n):
    out, bit = me, 1
    while bit < n:
        if not isinstance(m, int):
            out = out + ((m // bit) % 2) * (1 - 2 * ((me // bit) % 2)) * bit
        elif m // bit % 2:
            out = out + (bit - 2 * bit * ((me // bit) % 2))
        bit *= 2
    return out


def loop(start, stop, body, unroll=False):
    if unroll is True and stop - start <= 16:
        for i in range(start, stop):
            body(i)
        return

    def step(i, carry):
        body(i)
        return carry

    lax.fori_loop(start, stop, step, 0, unroll=unroll)


def pack_ids(q, most, vocab, zero_row, counts, xt, lt, ids_out):
    pooling = ids_out.shape[1]
    tabs = PACK_GROUP
    shape = (2 * pooling, LANES)
    sub, lane = iota(shape, 0), iota(shape, 1)
    high, p = sub >= pooling, sub % pooling
    first, second = 2 * q * tabs, (2 * q + 1) * tabs
    off_a, off_b = jnp.int32(0), jnp.int32(0)
    ids = jnp.full(shape, zero_row, I32)
    for t in range(tabs):
        count_a, count_b = counts[first + t], counts[second + t]
        unit = lane - jnp.where(high, off_b, off_a)
        at = jnp.clip(unit, 0, most - 1)
        rows = jnp.where(high, xt[pl.ds(second + t, 1), :], xt[pl.ds(first + t, 1), :])
        lengths = jnp.where(high, lt[pl.ds(second + t, 1), :], lt[pl.ds(first + t, 1), :])
        row = jnp.take_along_axis(rows, at * pooling + p, axis=1, mode="promise_in_bounds")
        length = jnp.take_along_axis(lengths, at, axis=1, mode="promise_in_bounds")
        used = (unit >= 0) & (unit < jnp.where(high, count_b, count_a)) & (p < length)
        ids = jnp.where(used, row + t * vocab, ids)
        off_a, off_b = off_a + count_a, off_b + count_b
    ids_out[2 * q] = ids[:pooling]
    ids_out[2 * q + 1] = ids[pooling:]


def place_targets(g, order, counts, inv, targets, expand):
    tabs = PACK_GROUP
    feature = iota((1, expand.shape[1]), 1)
    off = jnp.int32(0)
    for t in range(tabs):
        s = g * tabs + t
        count = counts[s]
        row = inv[pl.ds(order[s], 1), :]
        row = jnp.where(row < count, row + off, -1)
        targets[g, t:t + 1, :] = row
        targets[g, tabs + t:tabs + t + 1, :] = pltpu.roll(row, row.shape[1] - 4, 1)
        off = off + count
        hot = jnp.where(feature == order[s], 1.0, 0.0)
        expand[pl.ds(g * 2 * tabs + t, 1), :] = hot
        expand[pl.ds(g * 2 * tabs + tabs + t, 1), :] = hot


def choose_rows(target, choice, at):
    samples = target.shape[1]
    lane = iota((16, LANES), 1)
    pairs = [blk * 8 + b for blk in range(samples // 8) for b in range(4)]
    for i in range(0, len(pairs), 2):
        wide = jnp.concatenate(
            [jnp.broadcast_to(target[:, c:c + 1], (8, LANES)) for c in pairs[i:i + 2]], axis=0
        )
        choice[at, i * 8:i * 8 + 16, :] = jnp.where(wide == lane, 1.0, 0.0).astype(BF16)


def exchange_kernel(
    n, most, room,
    bags_hbm, lens_hbm, tables_hbm, inv_hbm, order_hbm, counts_hbm, compress_hbm, weight_hbm,
    f_ref, mixer_ref, w_ref,
    bags, lens, tab16, inv, order, counts, compress, weight,
    tab32, xt, lt, ids_out, ids_in, pooled, staging, rows, targets, expand, choice,
    local, own_sem, id_send, id_recv, row_send, row_recv,
):
    me = lax.axis_index("dev")
    tabs, vocab, width = tab16.shape
    slots, samples = inv.shape
    mixes = compress.shape[0]
    pooling = ids_out.shape[1]
    zero_row = tabs * vocab
    small = n <= 16

    barrier = pltpu.get_barrier_semaphore()
    loop(
        1, n,
        lambda m: pl.semaphore_signal(barrier, inc=1, device_id={"dev": flip(me, m, n)}),
        unroll=small,
    )

    copies = [
        pltpu.make_async_copy(src, dst, local.at[i])
        for i, (src, dst) in enumerate([
            (counts_hbm, counts), (bags_hbm, bags), (lens_hbm, lens), (order_hbm, order),
            (inv_hbm, inv), (compress_hbm, compress), (tables_hbm, tab16), (weight_hbm, weight),
        ])
    ]
    for copy in copies:
        copy.start()
    counts_in, bags_in, lens_in, order_in, inv_in, compress_in, tables_in, weight_in = copies

    bags_in.wait()
    xt[...] = bags[...].T
    lens_in.wait()
    lt[...] = jnp.concatenate(
        [lens[...], jnp.zeros((LANES - most, slots), I32)], axis=0
    ).T
    counts_in.wait()
    loop(
        0, n // 2, lambda q: pack_ids(q, most, vocab, zero_row, counts, xt, lt, ids_out),
        unroll=small,
    )
    pl.semaphore_wait(barrier, n - 1)

    def id_copy(m):
        peer = flip(me, m, n)
        return pltpu.make_async_remote_copy(
            src_ref=ids_out.at[peer], dst_ref=ids_in.at[m],
            send_sem=id_send.at[m], recv_sem=id_recv.at[m],
            device_id={"dev": peer},
        )

    def row_copy(m):
        peer = flip(me, m, n)
        return pltpu.make_async_remote_copy(
            src_ref=staging.at[m], dst_ref=rows.at[me],
            send_sem=row_send.at[m], recv_sem=row_recv.at[me],
            device_id={"dev": peer},
        )

    loop(1, n, lambda m: id_copy(m).start(), unroll=small)
    own_ids = pltpu.make_async_copy(ids_out.at[me], ids_in.at[0], own_sem)
    own_ids.start()

    tables_in.wait()
    tab32[pl.ds(zero_row, 8), :] = jnp.zeros((8, width), F32)
    step = 256

    def widen(i):
        for t in range(tabs):
            base = pl.multiple_of(i * step, step)
            tab32[pl.ds(t * vocab + base, step), :] = tab16[t, pl.ds(base, step), :].astype(F32)

    loop(0, vocab // step, widen)

    order_in.wait()
    inv_in.wait()
    loop(0, n, lambda g: place_targets(g, order, counts, inv, targets, expand), unroll=4)

    weight_in.wait()
    group = 8
    inner = group * mixes
    r, c = iota((inner, inner), 0), iota((inner, inner), 1)
    source = ((r // 8) % 2 * tabs + r % tabs) * mixes + 2 * (r // 16) + (r // 4) % 2
    reorder = jnp.where(c == source, 1.0, 0.0).astype(BF16)

    def order_weight(q):
        block = jnp.concatenate([weight[order[q * group + i]] for i in range(group)], axis=0)
        moved = jnp.dot(reorder, block, preferred_element_type=F32).astype(BF16)
        w_ref[:, pl.ds(pl.multiple_of(q * 16, 16), 16), :] = moved.reshape(mixes // 2, 16, -1)

    loop(0, slots // group, order_weight, unroll=4)

    compress_in.wait()
    across = f_ref.shape[1]
    spread = lax.dot_general(
        compress[...], expand[...].astype(BF16), (((1,), (1,)), ((), ())),
        preferred_element_type=F32,
    )
    sub, lane = iota((8, across), 0), iota((8, across), 1)
    same_half = (lane // tabs) % 2 == sub // 4
    for k in range(0, mixes, 2):
        for b in range(4):
            held = same_half & (sub % 4 == b)
            kept = [
                jnp.where(held, jnp.broadcast_to(spread[k + h:k + h + 1, :], (8, across)), 0.0)
                for h in range(2)
            ]
            mixer_ref[k * 8:k * 8 + 16, b * across:(b + 1) * across] = (
                jnp.concatenate(kept, axis=0).astype(BF16)
            )

    def pool(m, store):
        def row_block(i):
            at = pl.multiple_of(i * 16, 16)
            for r in range(16):
                total = None
                for p in range(pooling):
                    row = tab32[pl.ds(ids_in[m, p, at + r], 1), :]
                    total = row if total is None else total + row
                pooled[pl.ds(at + r, 1), :] = total

        loop(0, room // 16, row_block, unroll=True)
        store(pooled[...].astype(BF16))

    own_ids.wait()

    def store_own(value):
        rows[me] = value

    pool(0, store_own)

    def serve(m):
        id_copy(m).wait_recv()

        def store(value):
            staging[m] = value

        pool(m, store)
        row_copy(m).start()

    lax.fori_loop(1, n, lambda i, c: (serve(i), c)[1], 0, unroll=small)
    if small:
        loop(0, n, lambda g: choose_rows(targets[g], choice, g), unroll=4)

    def select(i):
        q = flip(me // 2, i, n // 2)
        features = []
        for h in range(2):
            g = 2 * q + h
            at = g
            if not small:
                at = h
                choose_rows(targets[g], choice, h)
            packed = jnp.concatenate([rows[g], jnp.zeros((LANES - room, width), BF16)], axis=0)
            chosen = jnp.dot(choice[at], packed, preferred_element_type=F32)
            features.append(chosen.reshape(samples // 2, 8, width))
        f_ref[:, pl.ds(pl.multiple_of(q * 16, 16), 16), :] = (
            jnp.concatenate(features, axis=1).astype(BF16)
        )

    def arrival(m):
        peer = flip(me, m, n)
        pltpu.make_async_remote_copy(
            src_ref=staging.at[m], dst_ref=rows.at[peer],
            send_sem=row_send.at[m], recv_sem=row_recv.at[peer],
            device_id={"dev": peer},
        ).wait_recv()

    arrival(1)
    select(0)

    def collect(i):
        arrival(2 * i)
        arrival(2 * i + 1)
        select(i)

    loop(1, n // 2, collect)

    def finish(m):
        id_copy(m).wait_send()
        row_copy(m).wait_send()

    loop(1, n, finish, unroll=small)


def exchange(n, bags, lens, tables, inv, order, counts, compress, weight):
    tabs, vocab, width = tables.shape
    rows, slots = bags.shape
    most = lens.shape[0]
    pooling = rows // most
    samples, mixes, units = inv.shape[1], compress.shape[0], weight.shape[-1]
    room = PACK_ROOM
    assert tabs == PACK_GROUP and pooling == 4 and rows == LANES and n & (n - 1) == 0
    across = 2 * slots
    held = 3 * tables.size * 2 + 3 * weight.size * 2 + 3 * n * room * width * 4
    held += (samples * across * width + min(n, 16) * 4 * samples * LANES) * 2
    in_hbm = pl.BlockSpec(memory_space=pltpu.HBM)
    vmem = pl.BlockSpec(memory_space=pltpu.VMEM)
    operands = [
        pltpu.with_memory_space_constraint(x, pltpu.HBM)
        for x in (bags, lens, tables, inv, order, counts, compress, weight)
    ]
    return pl.pallas_call(
        functools.partial(exchange_kernel, n, most, room),
        out_shape=[
            jax.ShapeDtypeStruct((samples // 2, across, width), BF16),
            jax.ShapeDtypeStruct((mixes * 8, 4 * across), BF16),
            jax.ShapeDtypeStruct((mixes // 2, across, units), BF16),
        ],
        in_specs=[in_hbm] * 8,
        out_specs=[vmem] * 3,
        scratch_shapes=[
            pltpu.VMEM(bags.shape, I32),
            pltpu.VMEM(lens.shape, I32),
            pltpu.VMEM(tables.shape, BF16),
            pltpu.VMEM(inv.shape, I32),
            pltpu.SMEM(order.shape, I32),
            pltpu.SMEM(counts.shape, I32),
            pltpu.VMEM(compress.shape, BF16),
            pltpu.VMEM(weight.shape, BF16),
            pltpu.VMEM((tabs * vocab + 8, width), F32),
            pltpu.VMEM((slots, LANES), I32),
            pltpu.VMEM((slots, LANES), I32),
            pltpu.VMEM((n, pooling, LANES), I32),
            pltpu.SMEM((n, pooling, LANES), I32),
            pltpu.VMEM((room, width), F32),
            pltpu.VMEM((n, room, width), BF16),
            pltpu.VMEM((n, room, width), BF16),
            pltpu.VMEM((n, 2 * tabs, samples), I32),
            pltpu.VMEM((across, slots), F32),
            pltpu.VMEM((n if n <= 16 else 2, 4 * samples, LANES), BF16),
            pltpu.SemaphoreType.DMA((8,)),
            pltpu.SemaphoreType.DMA,
            pltpu.SemaphoreType.DMA((n,)),
            pltpu.SemaphoreType.DMA((n,)),
            pltpu.SemaphoreType.DMA((n,)),
            pltpu.SemaphoreType.DMA((n,)),
        ],
        compiler_params=pltpu.CompilerParams(
            collective_id=0, has_side_effects=True, vmem_limit_bytes=min(63 << 20, held + (6 << 20))
        ),
        name="exchange",
    )(*operands)


def interact_kernel(f_ref, mixer_ref, w_ref, bias_ref, out_ref, pairs):
    across, width = f_ref.shape[1:]
    mixes = mixer_ref.shape[0] // 8
    samples = out_ref.shape[0]
    sub, lane = iota((8, across), 0), iota((8, across), 1)
    first = sub < 4
    in_place = (lane // 4) % 2 == sub // 4
    mine = [sub % 4 == b for b in range(4)]

    def block(j):
        features = f_ref[pl.ds(j * 4, 4)].reshape(4 * across, width)
        mixed = jnp.dot(mixer_ref[...], features, preferred_element_type=F32).astype(BF16)
        products = lax.dot_general(
            mixed, features, (((1,), (1,)), ((), ())), preferred_element_type=F32
        )

        def of_mixture(k):
            parts = products[k * 8:k * 8 + 8, :]
            out = parts[:, :across]
            for b in range(1, 4):
                out = jnp.where(mine[b], parts[:, b * across:(b + 1) * across], out)
            return out

        for k in range(0, mixes, 2):
            even, odd = of_mixture(k), of_mixture(k + 1)
            stay, move = jnp.where(first, even, odd), jnp.where(first, odd, even)
            moved = jnp.where(first, pltpu.roll(move, 4, 1), pltpu.roll(move, across - 4, 1))
            pairs[pl.ds(pl.multiple_of(j * 8, 8), 8), k // 2 * across:(k // 2 + 1) * across] = (
                jnp.where(in_place, stay, moved)
            )

    loop(0, samples // 8, block, unroll=samples <= LANES and across <= LANES)
    hidden = jnp.dot(
        pairs[...].astype(BF16), w_ref[...].reshape(mixes // 2 * across, -1),
        preferred_element_type=F32,
    ) + bias_ref[...]
    out_ref[...] = jnp.maximum(hidden, 0.0).astype(BF16)


def interact(features, mixer, weight, bias):
    pairs_of_samples, across, _ = features.shape
    samples, half_mixes, units = 2 * pairs_of_samples, weight.shape[0], weight.shape[2]
    held = (features.size + 2 * weight.size + mixer.size) * 2 + 6 * samples * half_mixes * across
    vmem = pl.BlockSpec(memory_space=pltpu.VMEM)
    return pl.pallas_call(
        interact_kernel,
        out_shape=jax.ShapeDtypeStruct((samples, units), BF16),
        in_specs=[vmem] * 4,
        out_specs=vmem,
        scratch_shapes=[pltpu.VMEM((samples, half_mixes * across), F32)],
        compiler_params=pltpu.CompilerParams(vmem_limit_bytes=min(63 << 20, held + (6 << 20))),
        name="interact",
    )(features, mixer, weight, bias)


def shards(
    n, tables, bag_rows, bag_lengths, row_counts, inverse, table_order, compress, top_weight, top_bias
):
    _, slots, most, pooling = bag_rows.shape
    mixes = compress.shape[0]
    features, mixer, weight = exchange(
        n, bag_rows[0].transpose(1, 2, 0).reshape(most * pooling, slots), bag_lengths[0].T, tables,
        inverse.T, table_order, row_counts[0], compress, top_weight.reshape(slots, mixes, -1),
    )
    return interact(features, mixer, weight, top_bias.reshape(1, -1))


def solution(mesh):
    return jax.shard_map(
        functools.partial(shards, mesh.shape["dev"]),
        mesh=mesh,
        in_specs=(
            P("dev", None, None),
            P(("rep", "dev"), None, None, None),
            P(("rep", "dev"), None, None),
            P(("rep", "dev"), None),
            P(("rep", "dev"), None),
            P(),
            P(),
            P(),
            P(),
        ),
        out_specs=P(("rep", "dev"), None),
        check_vma=False,
    )
```

```python
import functools

import jax
import jax.numpy as jnp
from jax import lax
from jax.experimental import pallas as pl
from jax.experimental.pallas import tpu as pltpu
from jax.sharding import PartitionSpec as P

F32 = jnp.float32
BF16 = jnp.bfloat16
I32 = jnp.int32
LANES = 128
PACK_GROUP, PACK_ROOM = 4, 80


def iota(shape, axis):
    return lax.broadcasted_iota(I32, shape, axis)


def flip(me, m, n):
    out, bit = me, 1
    while bit < n:
        if not isinstance(m, int):
            out = out + ((m // bit) % 2) * (1 - 2 * ((me // bit) % 2)) * bit
        elif m // bit % 2:
            out = out + (bit - 2 * bit * ((me // bit) % 2))
        bit *= 2
    return out


def loop(start, stop, body, unroll=False):
    if unroll is True and stop - start <= 16:
        for i in range(start, stop):
            body(i)
        return

    def step(i, carry):
        body(i)
        return carry

    lax.fori_loop(start, stop, step, 0, unroll=unroll)


def pack_ids(q, most, vocab, zero_row, counts, xt, lt, ids_out):
    pooling = ids_out.shape[1]
    tabs = PACK_GROUP
    shape = (2 * pooling, LANES)
    sub, lane = iota(shape, 0), iota(shape, 1)
    high, p = sub >= pooling, sub % pooling
    first, second = 2 * q * tabs, (2 * q + 1) * tabs
    off_a, off_b = jnp.int32(0), jnp.int32(0)
    ids = jnp.full(shape, zero_row, I32)
    for t in range(tabs):
        count_a, count_b = counts[first + t], counts[second + t]
        unit = lane - jnp.where(high, off_b, off_a)
        at = jnp.clip(unit, 0, most - 1)
        rows = jnp.where(high, xt[pl.ds(second + t, 1), :], xt[pl.ds(first + t, 1), :])
        lengths = jnp.where(high, lt[pl.ds(second + t, 1), :], lt[pl.ds(first + t, 1), :])
        row = jnp.take_along_axis(rows, at * pooling + p, axis=1, mode="promise_in_bounds")
        length = jnp.take_along_axis(lengths, at, axis=1, mode="promise_in_bounds")
        used = (unit >= 0) & (unit < jnp.where(high, count_b, count_a)) & (p < length)
        ids = jnp.where(used, row + t * vocab, ids)
        off_a, off_b = off_a + count_a, off_b + count_b
    ids_out[2 * q] = ids[:pooling]
    ids_out[2 * q + 1] = ids[pooling:]


def place_targets(g, order, counts, inv, targets, expand):
    tabs = PACK_GROUP
    feature = iota((1, expand.shape[1]), 1)
    off = jnp.int32(0)
    for t in range(tabs):
        s = g * tabs + t
        count = counts[s]
        row = inv[pl.ds(order[s], 1), :]
        row = jnp.where(row < count, row + off, -1)
        targets[g, t:t + 1, :] = row
        targets[g, tabs + t:tabs + t + 1, :] = pltpu.roll(row, row.shape[1] - 4, 1)
        off = off + count
        hot = jnp.where(feature == order[s], 1.0, 0.0)
        expand[pl.ds(g * 2 * tabs + t, 1), :] = hot
        expand[pl.ds(g * 2 * tabs + tabs + t, 1), :] = hot


def choose_rows(target, choice, at):
    samples = target.shape[1]
    lane = iota((16, LANES), 1)
    pairs = [blk * 8 + b for blk in range(samples // 8) for b in range(4)]
    for i in range(0, len(pairs), 2):
        wide = jnp.concatenate(
            [jnp.broadcast_to(target[:, c:c + 1], (8, LANES)) for c in pairs[i:i + 2]], axis=0
        )
        choice[at, i * 8:i * 8 + 16, :] = jnp.where(wide == lane, 1.0, 0.0).astype(BF16)


def exchange_kernel(
    n, most, room,
    bags_hbm, lens_hbm, tables_hbm, inv_hbm, order_hbm, counts_hbm, compress_hbm, weight_hbm,
    f_ref, mixer_ref, w_ref,
    bags, lens, tab16, inv, order, counts, compress, weight,
    tab32, xt, lt, ids_out, ids_in, pooled, staging, rows, targets, expand, choice,
    local, own_sem, id_send, id_recv, row_send, row_recv,
):
    me = lax.axis_index("dev")
    tabs, vocab, width = tab16.shape
    slots, samples = inv.shape
    mixes = compress.shape[0]
    pooling = ids_out.shape[1]
    zero_row = tabs * vocab
    small = n <= 16

    barrier = pltpu.get_barrier_semaphore()
    loop(
        1, n,
        lambda m: pl.semaphore_signal(barrier, inc=1, device_id={"dev": flip(me, m, n)}),
        unroll=small,
    )

    copies = [
        pltpu.make_async_copy(src, dst, local.at[i])
        for i, (src, dst) in enumerate([
            (counts_hbm, counts), (bags_hbm, bags), (lens_hbm, lens), (order_hbm, order),
            (inv_hbm, inv), (compress_hbm, compress), (tables_hbm, tab16), (weight_hbm, weight),
        ])
    ]
    for copy in copies:
        copy.start()
    counts_in, bags_in, lens_in, order_in, inv_in, compress_in, tables_in, weight_in = copies

    bags_in.wait()
    xt[...] = bags[...].T
    lens_in.wait()
    lt[...] = jnp.concatenate(
        [lens[...], jnp.zeros((LANES - most, slots), I32)], axis=0
    ).T
    counts_in.wait()
    loop(
        0, n // 2, lambda q: pack_ids(q, most, vocab, zero_row, counts, xt, lt, ids_out),
        unroll=small,
    )
    pl.semaphore_wait(barrier, n - 1)

    def id_copy(m):
        peer = flip(me, m, n)
        return pltpu.make_async_remote_copy(
            src_ref=ids_out.at[peer], dst_ref=ids_in.at[m],
            send_sem=id_send.at[m], recv_sem=id_recv.at[m],
            device_id={"dev": peer},
        )

    def row_copy(m):
        peer = flip(me, m, n)
        return pltpu.make_async_remote_copy(
            src_ref=staging.at[m], dst_ref=rows.at[me],
            send_sem=row_send.at[m], recv_sem=row_recv.at[me],
            device_id={"dev": peer},
        )

    loop(1, n, lambda m: id_copy(m).start(), unroll=small)
    own_ids = pltpu.make_async_copy(ids_out.at[me], ids_in.at[0], own_sem)
    own_ids.start()

    tables_in.wait()
    tab32[pl.ds(zero_row, 8), :] = jnp.zeros((8, width), F32)
    step = 256

    def widen(i):
        for t in range(tabs):
            base = pl.multiple_of(i * step, step)
            tab32[pl.ds(t * vocab + base, step), :] = tab16[t, pl.ds(base, step), :].astype(F32)

    loop(0, vocab // step, widen)

    order_in.wait()
    inv_in.wait()
    loop(0, n, lambda g: place_targets(g, order, counts, inv, targets, expand), unroll=4)

    weight_in.wait()
    group = 8
    inner = group * mixes
    r, c = iota((inner, inner), 0), iota((inner, inner), 1)
    source = ((r // 8) % 2 * tabs + r % tabs) * mixes + 2 * (r // 16) + (r // 4) % 2
    reorder = jnp.where(c == source, 1.0, 0.0).astype(BF16)

    def order_weight(q):
        block = jnp.concatenate([weight[order[q * group + i]] for i in range(group)], axis=0)
        moved = jnp.dot(reorder, block, preferred_element_type=F32).astype(BF16)
        w_ref[:, pl.ds(pl.multiple_of(q * 16, 16), 16), :] = moved.reshape(mixes // 2, 16, -1)

    loop(0, slots // group, order_weight, unroll=4)

    compress_in.wait()
    across = f_ref.shape[1]
    spread = lax.dot_general(
        compress[...], expand[...].astype(BF16), (((1,), (1,)), ((), ())),
        preferred_element_type=F32,
    )
    sub, lane = iota((8, across), 0), iota((8, across), 1)
    same_half = (lane // tabs) % 2 == sub // 4
    for k in range(0, mixes, 2):
        for b in range(4):
            held = same_half & (sub % 4 == b)
            kept = [
                jnp.where(held, jnp.broadcast_to(spread[k + h:k + h + 1, :], (8, across)), 0.0)
                for h in range(2)
            ]
            mixer_ref[k * 8:k * 8 + 16, b * across:(b + 1) * across] = (
                jnp.concatenate(kept, axis=0).astype(BF16)
            )

    def pool(m, store):
        def row_block(i):
            at = pl.multiple_of(i * 16, 16)
            for r in range(16):
                total = None
                for p in range(pooling):
                    row = tab32[pl.ds(ids_in[m, p, at + r], 1), :]
                    total = row if total is None else total + row
                pooled[pl.ds(at + r, 1), :] = total

        loop(0, room // 16, row_block, unroll=True)
        store(pooled[...].astype(BF16))

    own_ids.wait()

    def store_own(value):
        rows[me] = value

    pool(0, store_own)

    def serve(m):
        id_copy(m).wait_recv()

        def store(value):
            staging[m] = value

        pool(m, store)
        row_copy(m).start()

    lax.fori_loop(1, n, lambda i, c: (serve(i), c)[1], 0, unroll=small)
    if small:
        loop(0, n, lambda g: choose_rows(targets[g], choice, g), unroll=4)

    def select(i):
        q = flip(me // 2, i, n // 2)
        features = []
        for h in range(2):
            g = 2 * q + h
            at = g
            if not small:
                at = h
                choose_rows(targets[g], choice, h)
            packed = jnp.concatenate([rows[g], jnp.zeros((LANES - room, width), BF16)], axis=0)
            chosen = jnp.dot(choice[at], packed, preferred_element_type=F32)
            features.append(chosen.reshape(samples // 2, 8, width))
        f_ref[:, pl.ds(pl.multiple_of(q * 16, 16), 16), :] = (
            jnp.concatenate(features, axis=1).astype(BF16)
        )

    def arrival(m):
        peer = flip(me, m, n)
        pltpu.make_async_remote_copy(
            src_ref=staging.at[m], dst_ref=rows.at[peer],
            send_sem=row_send.at[m], recv_sem=row_recv.at[peer],
            device_id={"dev": peer},
        ).wait_recv()

    arrival(1)
    select(0)

    def collect(i):
        arrival(2 * i)
        arrival(2 * i + 1)
        select(i)

    loop(1, n // 2, collect)

    def finish(m):
        id_copy(m).wait_send()
        row_copy(m).wait_send()

    loop(1, n, finish, unroll=small)


def exchange(n, bags, lens, tables, inv, order, counts, compress, weight):
    tabs, vocab, width = tables.shape
    rows, slots = bags.shape
    most = lens.shape[0]
    pooling = rows // most
    samples, mixes, units = inv.shape[1], compress.shape[0], weight.shape[-1]
    room = PACK_ROOM
    assert tabs == PACK_GROUP and pooling == 4 and rows == LANES and n & (n - 1) == 0
    across = 2 * slots
    held = 3 * tables.size * 2 + 3 * weight.size * 2 + 3 * n * room * width * 4
    held += (samples * across * width + min(n, 16) * 4 * samples * LANES) * 2
    in_hbm = pl.BlockSpec(memory_space=pltpu.HBM)
    vmem = pl.BlockSpec(memory_space=pltpu.VMEM)
    operands = [
        pltpu.with_memory_space_constraint(x, pltpu.HBM)
        for x in (bags, lens, tables, inv, order, counts, compress, weight)
    ]
    return pl.pallas_call(
        functools.partial(exchange_kernel, n, most, room),
        out_shape=[
            jax.ShapeDtypeStruct((samples // 2, across, width), BF16),
            jax.ShapeDtypeStruct((mixes * 8, 4 * across), BF16),
            jax.ShapeDtypeStruct((mixes // 2, across, units), BF16),
        ],
        in_specs=[in_hbm] * 8,
        out_specs=[vmem] * 3,
        scratch_shapes=[
            pltpu.VMEM(bags.shape, I32),
            pltpu.VMEM(lens.shape, I32),
            pltpu.VMEM(tables.shape, BF16),
            pltpu.VMEM(inv.shape, I32),
            pltpu.SMEM(order.shape, I32),
            pltpu.SMEM(counts.shape, I32),
            pltpu.VMEM(compress.shape, BF16),
            pltpu.VMEM(weight.shape, BF16),
            pltpu.VMEM((tabs * vocab + 8, width), F32),
            pltpu.VMEM((slots, LANES), I32),
            pltpu.VMEM((slots, LANES), I32),
            pltpu.VMEM((n, pooling, LANES), I32),
            pltpu.SMEM((n, pooling, LANES), I32),
            pltpu.VMEM((room, width), F32),
            pltpu.VMEM((n, room, width), BF16),
            pltpu.VMEM((n, room, width), BF16),
            pltpu.VMEM((n, 2 * tabs, samples), I32),
            pltpu.VMEM((across, slots), F32),
            pltpu.VMEM((n if n <= 16 else 2, 4 * samples, LANES), BF16),
            pltpu.SemaphoreType.DMA((8,)),
            pltpu.SemaphoreType.DMA,
            pltpu.SemaphoreType.DMA((n,)),
            pltpu.SemaphoreType.DMA((n,)),
            pltpu.SemaphoreType.DMA((n,)),
            pltpu.SemaphoreType.DMA((n,)),
        ],
        compiler_params=pltpu.CompilerParams(
            collective_id=0, has_side_effects=True, vmem_limit_bytes=min(63 << 20, held + (6 << 20))
        ),
        name="exchange",
    )(*operands)


def interact_kernel(f_ref, mixer_ref, w_ref, bias_ref, out_ref, pairs):
    across, width = f_ref.shape[1:]
    mixes = mixer_ref.shape[0] // 8
    samples = out_ref.shape[0]
    sub, lane = iota((8, across), 0), iota((8, across), 1)
    first = sub < 4
    in_place = (lane // 4) % 2 == sub // 4
    mine = [sub % 4 == b for b in range(4)]

    def block(j, features, mixed):
        products = lax.dot_general(
            mixed, features, (((1,), (1,)), ((), ())), preferred_element_type=F32
        )

        def of_mixture(k):
            parts = products[k * 8:k * 8 + 8, :]
            out = parts[:, :across]
            for b in range(1, 4):
                out = jnp.where(mine[b], parts[:, b * across:(b + 1) * across], out)
            return out

        for k in range(0, mixes, 2):
            even, odd = of_mixture(k), of_mixture(k + 1)
            stay, move = jnp.where(first, even, odd), jnp.where(first, odd, even)
            moved = jnp.where(first, pltpu.roll(move, 4, 1), pltpu.roll(move, across - 4, 1))
            pairs[pl.ds(pl.multiple_of(j * 8, 8), 8), k // 2 * across:(k // 2 + 1) * across] = (
                jnp.where(in_place, stay, moved)
            )

    def two_blocks(i):
        features = [f_ref[pl.ds(i * 8 + h * 4, 4)].reshape(4 * across, width) for h in range(2)]
        mixed = jnp.dot(
            mixer_ref[...], jnp.concatenate(features, axis=1), preferred_element_type=F32
        ).astype(BF16)
        for h in range(2):
            block(2 * i + h, features[h], mixed[:, h * width:(h + 1) * width])

    loop(0, samples // 16, two_blocks, unroll=samples <= LANES and across <= LANES)
    hidden = jnp.dot(
        pairs[...].astype(BF16), w_ref[...].reshape(mixes // 2 * across, -1),
        preferred_element_type=F32,
    ) + bias_ref[...]
    out_ref[...] = jnp.maximum(hidden, 0.0).astype(BF16)


def interact(features, mixer, weight, bias):
    pairs_of_samples, across, _ = features.shape
    samples, half_mixes, units = 2 * pairs_of_samples, weight.shape[0], weight.shape[2]
    held = (features.size + 2 * weight.size + mixer.size) * 2 + 6 * samples * half_mixes * across
    vmem = pl.BlockSpec(memory_space=pltpu.VMEM)
    return pl.pallas_call(
        interact_kernel,
        out_shape=jax.ShapeDtypeStruct((samples, units), BF16),
        in_specs=[vmem] * 4,
        out_specs=vmem,
        scratch_shapes=[pltpu.VMEM((samples, half_mixes * across), F32)],
        compiler_params=pltpu.CompilerParams(vmem_limit_bytes=min(63 << 20, held + (6 << 20))),
        name="interact",
    )(features, mixer, weight, bias)


def shards(
    n, tables, bag_rows, bag_lengths, row_counts, inverse, table_order, compress, top_weight, top_bias
):
    _, slots, most, pooling = bag_rows.shape
    mixes = compress.shape[0]
    features, mixer, weight = exchange(
        n, bag_rows[0].transpose(1, 2, 0).reshape(most * pooling, slots), bag_lengths[0].T, tables,
        inverse.T, table_order, row_counts[0], compress, top_weight.reshape(slots, mixes, -1),
    )
    return interact(features, mixer, weight, top_bias.reshape(1, -1))


def solution(mesh):
    return jax.shard_map(
        functools.partial(shards, mesh.shape["dev"]),
        mesh=mesh,
        in_specs=(
            P("dev", None, None),
            P(("rep", "dev"), None, None, None),
            P(("rep", "dev"), None, None),
            P(("rep", "dev"), None),
            P(("rep", "dev"), None),
            P(),
            P(),
            P(),
            P(),
        ),
        out_specs=P(("rep", "dev"), None),
        check_vma=False,
    )
```

```python
import functools

import jax
import jax.numpy as jnp
from jax import lax
from jax.experimental import pallas as pl
from jax.experimental.pallas import tpu as pltpu
from jax.sharding import PartitionSpec as P

F32 = jnp.float32
BF16 = jnp.bfloat16
I32 = jnp.int32
LANES = 128
PACK_GROUP, PACK_ROOM = 4, 80


def iota(shape, axis):
    return lax.broadcasted_iota(I32, shape, axis)


def flip(me, m, n):
    out, bit = me, 1
    while bit < n:
        if not isinstance(m, int):
            out = out + ((m // bit) % 2) * (1 - 2 * ((me // bit) % 2)) * bit
        elif m // bit % 2:
            out = out + (bit - 2 * bit * ((me // bit) % 2))
        bit *= 2
    return out


def turn(m, device, n, back=False):
    def place(m):
        return (m - 12 + n - 1) % (n - 1) + 1

    hops = device % 2 + (device // 2) % 2 + device // 4
    early, late = jnp.clip((5 * hops - 3) // 2, 1, n - 1), place(device)
    at = m if back else place(m)
    moved = jnp.where(at == late, early, jnp.where(at == early, late, at))
    at = jnp.where(device == 0, at, moved)
    return (at - 1 + 12 - 1) % (n - 1) + 1 if back else at


def loop(start, stop, body, unroll=False):
    if unroll is True and stop - start <= 16:
        for i in range(start, stop):
            body(i)
        return

    def step(i, carry):
        body(i)
        return carry

    lax.fori_loop(start, stop, step, 0, unroll=unroll)


def pack_ids(q, most, vocab, zero_row, counts, xt, lt, ids_out):
    pooling = ids_out.shape[1]
    tabs = PACK_GROUP
    shape = (2 * pooling, LANES)
    sub, lane = iota(shape, 0), iota(shape, 1)
    high, p = sub >= pooling, sub % pooling
    first, second = 2 * q * tabs, (2 * q + 1) * tabs
    off_a, off_b = jnp.int32(0), jnp.int32(0)
    ids = jnp.full(shape, zero_row, I32)
    for t in range(tabs):
        count_a, count_b = counts[first + t], counts[second + t]
        unit = lane - jnp.where(high, off_b, off_a)
        at = jnp.clip(unit, 0, most - 1)
        rows = jnp.where(high, xt[pl.ds(second + t, 1), :], xt[pl.ds(first + t, 1), :])
        lengths = jnp.where(high, lt[pl.ds(second + t, 1), :], lt[pl.ds(first + t, 1), :])
        row = jnp.take_along_axis(rows, at * pooling + p, axis=1, mode="promise_in_bounds")
        length = jnp.take_along_axis(lengths, at, axis=1, mode="promise_in_bounds")
        used = (unit >= 0) & (unit < jnp.where(high, count_b, count_a)) & (p < length)
        ids = jnp.where(used, row + t * vocab, ids)
        off_a, off_b = off_a + count_a, off_b + count_b
    ids_out[2 * q] = ids[:pooling]
    ids_out[2 * q + 1] = ids[pooling:]


def place_targets(g, order, counts, inv, targets, expand):
    tabs = PACK_GROUP
    feature = iota((1, expand.shape[1]), 1)
    off = jnp.int32(0)
    for t in range(tabs):
        s = g * tabs + t
        count = counts[s]
        row = inv[pl.ds(order[s], 1), :]
        row = jnp.where(row < count, row + off, -1)
        targets[g, t:t + 1, :] = row
        targets[g, tabs + t:tabs + t + 1, :] = pltpu.roll(row, row.shape[1] - 4, 1)
        off = off + count
        hot = jnp.where(feature == order[s], 1.0, 0.0)
        expand[pl.ds(g * 2 * tabs + t, 1), :] = hot
        expand[pl.ds(g * 2 * tabs + tabs + t, 1), :] = hot


def choose_rows(target, choice, at):
    samples = target.shape[1]
    lane = iota((16, LANES), 1)
    pairs = [blk * 8 + b for blk in range(samples // 8) for b in range(4)]
    for i in range(0, len(pairs), 2):
        wide = jnp.concatenate(
            [jnp.broadcast_to(target[:, c:c + 1], (8, LANES)) for c in pairs[i:i + 2]], axis=0
        )
        choice[at, i * 8:i * 8 + 16, :] = jnp.where(wide == lane, 1.0, 0.0).astype(BF16)


def exchange_kernel(
    n, most, room,
    bags_hbm, lens_hbm, tables_hbm, inv_hbm, order_hbm, counts_hbm, compress_hbm, weight_hbm,
    f_ref, mixer_ref, w_ref,
    bags, lens, tab16, inv, order, counts, compress, weight,
    tab32, xt, lt, ids_out, ids_in, pooled, staging, rows, targets, expand, choice,
    local, own_sem, id_send, id_recv, row_send, row_recv,
):
    me = lax.axis_index("dev")
    tabs, vocab, width = tab16.shape
    slots, samples = inv.shape
    mixes = compress.shape[0]
    pooling = ids_out.shape[1]
    zero_row = tabs * vocab
    small = n <= 16

    barrier = pltpu.get_barrier_semaphore()
    loop(
        1, n,
        lambda i: pl.semaphore_signal(barrier, inc=1, device_id={"dev": flip(me, n - i, n)}),
        unroll=small,
    )

    copies = [
        pltpu.make_async_copy(src, dst, local.at[i])
        for i, (src, dst) in enumerate([
            (counts_hbm, counts), (bags_hbm, bags), (lens_hbm, lens), (order_hbm, order),
            (inv_hbm, inv), (compress_hbm, compress), (tables_hbm, tab16), (weight_hbm, weight),
        ])
    ]
    for copy in copies:
        copy.start()
    counts_in, bags_in, lens_in, order_in, inv_in, compress_in, tables_in, weight_in = copies

    bags_in.wait()
    xt[...] = bags[...].T
    lens_in.wait()
    lt[...] = jnp.concatenate(
        [lens[...], jnp.zeros((LANES - most, slots), I32)], axis=0
    ).T
    counts_in.wait()
    loop(
        0, n // 2, lambda q: pack_ids(q, most, vocab, zero_row, counts, xt, lt, ids_out),
        unroll=small,
    )
    pl.semaphore_wait(barrier, n - 1)

    def id_copy(m):
        peer = flip(me, m, n)
        return pltpu.make_async_remote_copy(
            src_ref=ids_out.at[peer], dst_ref=ids_in.at[turn(m, peer, n)],
            send_sem=id_send.at[m], recv_sem=id_recv.at[turn(m, peer, n)],
            device_id={"dev": peer},
        )

    def id_arrival(m):
        peer = flip(me, turn(m, me, n, True), n)
        return pltpu.make_async_remote_copy(
            src_ref=ids_out.at[peer], dst_ref=ids_in.at[m],
            send_sem=id_send.at[m], recv_sem=id_recv.at[m],
            device_id={"dev": peer},
        )

    def row_copy(m):
        peer = flip(me, turn(m, me, n, True), n)
        return pltpu.make_async_remote_copy(
            src_ref=staging.at[m], dst_ref=rows.at[me],
            send_sem=row_send.at[m], recv_sem=row_recv.at[me],
            device_id={"dev": peer},
        )

    loop(1, n, lambda i: id_copy(n - i).start(), unroll=small)
    own_ids = pltpu.make_async_copy(ids_out.at[me], ids_in.at[0], own_sem)
    own_ids.start()

    tables_in.wait()
    tab32[pl.ds(zero_row, 8), :] = jnp.zeros((8, width), F32)
    step = 256

    def widen(i):
        for t in range(tabs):
            base = pl.multiple_of(i * step, step)
            tab32[pl.ds(t * vocab + base, step), :] = tab16[t, pl.ds(base, step), :].astype(F32)

    loop(0, vocab // step, widen)

    order_in.wait()
    inv_in.wait()
    loop(0, n, lambda g: place_targets(g, order, counts, inv, targets, expand), unroll=4)

    weight_in.wait()
    group = 8
    inner = group * mixes
    r, c = iota((inner, inner), 0), iota((inner, inner), 1)
    source = ((r // 8) % 2 * tabs + r % tabs) * mixes + 2 * (r // 16) + (r // 4) % 2
    reorder = jnp.where(c == source, 1.0, 0.0).astype(BF16)

    def order_weight(q):
        block = jnp.concatenate([weight[order[q * group + i]] for i in range(group)], axis=0)
        moved = jnp.dot(reorder, block, preferred_element_type=F32).astype(BF16)
        w_ref[:, pl.ds(pl.multiple_of(q * 16, 16), 16), :] = moved.reshape(mixes // 2, 16, -1)

    loop(0, slots // group, order_weight, unroll=4)

    compress_in.wait()
    across = f_ref.shape[1]
    spread = lax.dot_general(
        compress[...], expand[...].astype(BF16), (((1,), (1,)), ((), ())),
        preferred_element_type=F32,
    )
    sub, lane = iota((8, across), 0), iota((8, across), 1)
    same_half = (lane // tabs) % 2 == sub // 4
    for k in range(0, mixes, 2):
        for b in range(4):
            held = same_half & (sub % 4 == b)
            kept = [
                jnp.where(held, jnp.broadcast_to(spread[k + h:k + h + 1, :], (8, across)), 0.0)
                for h in range(2)
            ]
            mixer_ref[k * 8:k * 8 + 16, b * across:(b + 1) * across] = (
                jnp.concatenate(kept, axis=0).astype(BF16)
            )

    def pool(m, store):
        def row_block(i):
            at = pl.multiple_of(i * 16, 16)
            for r in range(16):
                total = None
                for p in range(pooling):
                    row = tab32[pl.ds(ids_in[m, p, at + r], 1), :]
                    total = row if total is None else total + row
                pooled[pl.ds(at + r, 1), :] = total

        loop(0, room // 16, row_block, unroll=True)
        store(pooled[...].astype(BF16))

    def store_own(value):
        rows[me] = value

    def serve(m):
        id_arrival(m).wait_recv()

        def store(value):
            staging[m] = value

        pool(m, store)
        row_copy(m).start()

    lax.fori_loop(1, n, lambda i, c: (serve(i), c)[1], 0, unroll=small)
    own_ids.wait()
    pool(0, store_own)
    if small:
        loop(0, n, lambda g: choose_rows(targets[g], choice, g), unroll=4)

    def select(i):
        q = flip(me // 2, i, n // 2)
        features = []
        for h in range(2):
            g = 2 * q + h
            at = g
            if not small:
                at = h
                choose_rows(targets[g], choice, h)
            packed = jnp.concatenate([rows[g], jnp.zeros((LANES - room, width), BF16)], axis=0)
            chosen = jnp.dot(choice[at], packed, preferred_element_type=F32)
            features.append(chosen.reshape(samples // 2, 8, width))
        f_ref[:, pl.ds(pl.multiple_of(q * 16, 16), 16), :] = (
            jnp.concatenate(features, axis=1).astype(BF16)
        )

    def arrival(m):
        peer = flip(me, m, n)
        pltpu.make_async_remote_copy(
            src_ref=staging.at[m], dst_ref=rows.at[peer],
            send_sem=row_send.at[m], recv_sem=row_recv.at[peer],
            device_id={"dev": peer},
        ).wait_recv()

    arrival(1)
    select(0)

    def collect(i):
        arrival(2 * i)
        arrival(2 * i + 1)
        select(i)

    loop(1, n // 2, collect)

    def finish(m):
        id_copy(m).wait_send()
        row_copy(m).wait_send()

    loop(1, n, finish, unroll=small)


def exchange(n, bags, lens, tables, inv, order, counts, compress, weight):
    tabs, vocab, width = tables.shape
    rows, slots = bags.shape
    most = lens.shape[0]
    pooling = rows // most
    samples, mixes, units = inv.shape[1], compress.shape[0], weight.shape[-1]
    room = PACK_ROOM
    assert tabs == PACK_GROUP and pooling == 4 and rows == LANES and n & (n - 1) == 0
    across = 2 * slots
    held = 3 * tables.size * 2 + 3 * weight.size * 2 + 3 * n * room * width * 4
    held += (samples * across * width + min(n, 16) * 4 * samples * LANES) * 2
    in_hbm = pl.BlockSpec(memory_space=pltpu.HBM)
    vmem = pl.BlockSpec(memory_space=pltpu.VMEM)
    operands = [
        pltpu.with_memory_space_constraint(x, pltpu.HBM)
        for x in (bags, lens, tables, inv, order, counts, compress, weight)
    ]
    return pl.pallas_call(
        functools.partial(exchange_kernel, n, most, room),
        out_shape=[
            jax.ShapeDtypeStruct((samples // 2, across, width), BF16),
            jax.ShapeDtypeStruct((mixes * 8, 4 * across), BF16),
            jax.ShapeDtypeStruct((mixes // 2, across, units), BF16),
        ],
        in_specs=[in_hbm] * 8,
        out_specs=[vmem] * 3,
        scratch_shapes=[
            pltpu.VMEM(bags.shape, I32),
            pltpu.VMEM(lens.shape, I32),
            pltpu.VMEM(tables.shape, BF16),
            pltpu.VMEM(inv.shape, I32),
            pltpu.SMEM(order.shape, I32),
            pltpu.SMEM(counts.shape, I32),
            pltpu.VMEM(compress.shape, BF16),
            pltpu.VMEM(weight.shape, BF16),
            pltpu.VMEM((tabs * vocab + 8, width), F32),
            pltpu.VMEM((slots, LANES), I32),
            pltpu.VMEM((slots, LANES), I32),
            pltpu.VMEM((n, pooling, LANES), I32),
            pltpu.SMEM((n, pooling, LANES), I32),
            pltpu.VMEM((room, width), F32),
            pltpu.VMEM((n, room, width), BF16),
            pltpu.VMEM((n, room, width), BF16),
            pltpu.VMEM((n, 2 * tabs, samples), I32),
            pltpu.VMEM((across, slots), F32),
            pltpu.VMEM((n if n <= 16 else 2, 4 * samples, LANES), BF16),
            pltpu.SemaphoreType.DMA((8,)),
            pltpu.SemaphoreType.DMA,
            pltpu.SemaphoreType.DMA((n,)),
            pltpu.SemaphoreType.DMA((n,)),
            pltpu.SemaphoreType.DMA((n,)),
            pltpu.SemaphoreType.DMA((n,)),
        ],
        compiler_params=pltpu.CompilerParams(
            collective_id=0, has_side_effects=True, vmem_limit_bytes=min(63 << 20, held + (6 << 20))
        ),
        name="exchange",
    )(*operands)


def interact_kernel(f_ref, mixer_ref, w_ref, bias_ref, out_ref, pairs):
    across, width = f_ref.shape[1:]
    mixes = mixer_ref.shape[0] // 8
    samples = out_ref.shape[0]
    sub, lane = iota((8, across), 0), iota((8, across), 1)
    first = sub < 4
    in_place = (lane // 4) % 2 == sub // 4
    mine = [sub % 4 == b for b in range(4)]

    def block(j, features, mixed):
        products = lax.dot_general(
            mixed, features, (((1,), (1,)), ((), ())), preferred_element_type=F32
        )

        def of_mixture(k):
            parts = products[k * 8:k * 8 + 8, :]
            out = parts[:, :across]
            for b in range(1, 4):
                out = jnp.where(mine[b], parts[:, b * across:(b + 1) * across], out)
            return out

        for k in range(0, mixes, 2):
            even, odd = of_mixture(k), of_mixture(k + 1)
            stay, move = jnp.where(first, even, odd), jnp.where(first, odd, even)
            moved = jnp.where(first, pltpu.roll(move, 4, 1), pltpu.roll(move, across - 4, 1))
            pairs[pl.ds(pl.multiple_of(j * 8, 8), 8), k // 2 * across:(k // 2 + 1) * across] = (
                jnp.where(in_place, stay, moved)
            )

    def two_blocks(i):
        features = [f_ref[pl.ds(i * 8 + h * 4, 4)].reshape(4 * across, width) for h in range(2)]
        mixed = jnp.dot(
            mixer_ref[...], jnp.concatenate(features, axis=1), preferred_element_type=F32
        ).astype(BF16)
        for h in range(2):
            block(2 * i + h, features[h], mixed[:, h * width:(h + 1) * width])

    loop(0, samples // 16, two_blocks, unroll=samples <= LANES and across <= LANES)
    hidden = jnp.dot(
        pairs[...].astype(BF16), w_ref[...].reshape(mixes // 2 * across, -1),
        preferred_element_type=F32,
    ) + bias_ref[...]
    out_ref[...] = jnp.maximum(hidden, 0.0).astype(BF16)


def interact(features, mixer, weight, bias):
    pairs_of_samples, across, _ = features.shape
    samples, half_mixes, units = 2 * pairs_of_samples, weight.shape[0], weight.shape[2]
    held = (features.size + 2 * weight.size + mixer.size) * 2 + 6 * samples * half_mixes * across
    vmem = pl.BlockSpec(memory_space=pltpu.VMEM)
    return pl.pallas_call(
        interact_kernel,
        out_shape=jax.ShapeDtypeStruct((samples, units), BF16),
        in_specs=[vmem] * 4,
        out_specs=vmem,
        scratch_shapes=[pltpu.VMEM((samples, half_mixes * across), F32)],
        compiler_params=pltpu.CompilerParams(vmem_limit_bytes=min(63 << 20, held + (6 << 20))),
        name="interact",
    )(features, mixer, weight, bias)


def shards(
    n, tables, bag_rows, bag_lengths, row_counts, inverse, table_order, compress, top_weight, top_bias
):
    _, slots, most, pooling = bag_rows.shape
    mixes = compress.shape[0]
    features, mixer, weight = exchange(
        n, bag_rows[0].transpose(1, 2, 0).reshape(most * pooling, slots), bag_lengths[0].T, tables,
        inverse.T, table_order, row_counts[0], compress, top_weight.reshape(slots, mixes, -1),
    )
    return interact(features, mixer, weight, top_bias.reshape(1, -1))


def solution(mesh):
    return jax.shard_map(
        functools.partial(shards, mesh.shape["dev"]),
        mesh=mesh,
        in_specs=(
            P("dev", None, None),
            P(("rep", "dev"), None, None, None),
            P(("rep", "dev"), None, None),
            P(("rep", "dev"), None),
            P(("rep", "dev"), None),
            P(),
            P(),
            P(),
            P(),
        ),
        out_specs=P(("rep", "dev"), None),
        check_vma=False,
    )
```

```python
import functools

import jax
import jax.numpy as jnp
from jax import lax
from jax.experimental import pallas as pl
from jax.experimental.pallas import tpu as pltpu
from jax.sharding import PartitionSpec as P

F32 = jnp.float32
BF16 = jnp.bfloat16
I32 = jnp.int32
LANES = 128
PACK_GROUP, PACK_ROOM = 4, 80


def iota(shape, axis):
    return lax.broadcasted_iota(I32, shape, axis)


def flip(me, m, n):
    out, bit = me, 1
    while bit < n:
        if not isinstance(m, int):
            out = out + ((m // bit) % 2) * (1 - 2 * ((me // bit) % 2)) * bit
        elif m // bit % 2:
            out = out + (bit - 2 * bit * ((me // bit) % 2))
        bit *= 2
    return out


def turn(m, device, n, back=False):
    def place(m):
        return (m - 12 + n - 1) % (n - 1) + 1

    hops = device % 2 + (device // 2) % 2 + device // 4
    early, late = jnp.clip((5 * hops - 3) // 2, 1, n - 1), place(device)
    at = m if back else place(m)
    moved = jnp.where(at == late, early, jnp.where(at == early, late, at))
    at = jnp.where(device == 0, at, moved)
    return (at - 1 + 12 - 1) % (n - 1) + 1 if back else at


def loop(start, stop, body, unroll=False):
    if unroll is True and stop - start <= 16:
        for i in range(start, stop):
            body(i)
        return

    def step(i, carry):
        body(i)
        return carry

    lax.fori_loop(start, stop, step, 0, unroll=unroll)


def pack_ids(q, most, vocab, zero_row, counts, xt, lt, ids_out):
    pooling = ids_out.shape[1]
    tabs = PACK_GROUP
    shape = (2 * pooling, LANES)
    sub, lane = iota(shape, 0), iota(shape, 1)
    high, p = sub >= pooling, sub % pooling
    first, second = 2 * q * tabs, (2 * q + 1) * tabs
    off_a, off_b = jnp.int32(0), jnp.int32(0)
    ids = jnp.full(shape, zero_row, I32)
    for t in range(tabs):
        count_a, count_b = counts[first + t], counts[second + t]
        unit = lane - jnp.where(high, off_b, off_a)
        at = jnp.clip(unit, 0, most - 1)
        rows = jnp.where(high, xt[pl.ds(second + t, 1), :], xt[pl.ds(first + t, 1), :])
        lengths = jnp.where(high, lt[pl.ds(second + t, 1), :], lt[pl.ds(first + t, 1), :])
        row = jnp.take_along_axis(rows, at * pooling + p, axis=1, mode="promise_in_bounds")
        length = jnp.take_along_axis(lengths, at, axis=1, mode="promise_in_bounds")
        used = (unit >= 0) & (unit < jnp.where(high, count_b, count_a)) & (p < length)
        ids = jnp.where(used, row + t * vocab, ids)
        off_a, off_b = off_a + count_a, off_b + count_b
    ids_out[2 * q] = ids[:pooling]
    ids_out[2 * q + 1] = ids[pooling:]


def place_targets(g, order, counts, inv, targets, expand):
    tabs = PACK_GROUP
    feature = iota((1, expand.shape[1]), 1)
    off = jnp.int32(0)
    for t in range(tabs):
        s = g * tabs + t
        count = counts[s]
        row = inv[pl.ds(order[s], 1), :]
        row = jnp.where(row < count, row + off, -1)
        targets[g, t:t + 1, :] = row
        targets[g, tabs + t:tabs + t + 1, :] = pltpu.roll(row, row.shape[1] - 4, 1)
        off = off + count
        hot = jnp.where(feature == order[s], 1.0, 0.0)
        expand[pl.ds(g * 2 * tabs + t, 1), :] = hot
        expand[pl.ds(g * 2 * tabs + tabs + t, 1), :] = hot


def choose_rows(target, choice, at):
    samples = target.shape[1]
    lane = iota((16, LANES), 1)
    pairs = [blk * 8 + b for blk in range(samples // 8) for b in range(4)]
    for i in range(0, len(pairs), 2):
        wide = jnp.concatenate(
            [jnp.broadcast_to(target[:, c:c + 1], (8, LANES)) for c in pairs[i:i + 2]], axis=0
        )
        choice[at, i * 8:i * 8 + 16, :] = jnp.where(wide == lane, 1.0, 0.0).astype(BF16)


def exchange_kernel(
    n, most, room,
    bags_hbm, lens_hbm, tables_hbm, inv_hbm, order_hbm, counts_hbm, compress_hbm, weight_hbm,
    f_ref, mixer_ref, w_ref,
    bags, lens, tab16, inv, order, counts, compress, weight,
    tab32, xt, lt, ids_out, ids_in, pooled, staging, rows, targets, expand, choice,
    local, own_sem, id_send, id_recv, row_send, row_recv,
):
    me = lax.axis_index("dev")
    tabs, vocab, width = tab16.shape
    slots, samples = inv.shape
    mixes = compress.shape[0]
    pooling = ids_out.shape[1]
    zero_row = tabs * vocab
    small = n <= 16

    barrier = pltpu.get_barrier_semaphore()
    loop(
        1, n,
        lambda i: pl.semaphore_signal(barrier, inc=1, device_id={"dev": flip(me, n - i, n)}),
        unroll=small,
    )

    copies = [
        pltpu.make_async_copy(src, dst, local.at[i])
        for i, (src, dst) in enumerate([
            (counts_hbm, counts), (bags_hbm, bags), (lens_hbm, lens), (order_hbm, order),
            (inv_hbm, inv), (compress_hbm, compress), (tables_hbm, tab16), (weight_hbm, weight),
        ])
    ]
    for copy in copies:
        copy.start()
    counts_in, bags_in, lens_in, order_in, inv_in, compress_in, tables_in, weight_in = copies

    bags_in.wait()
    xt[...] = bags[...].T
    lens_in.wait()
    lt[...] = jnp.concatenate(
        [lens[...], jnp.zeros((LANES - most, slots), I32)], axis=0
    ).T
    counts_in.wait()
    loop(
        0, n // 2, lambda q: pack_ids(q, most, vocab, zero_row, counts, xt, lt, ids_out),
        unroll=small,
    )
    pl.semaphore_wait(barrier, n - 1)

    def id_copy(m):
        peer = flip(me, m, n)
        return pltpu.make_async_remote_copy(
            src_ref=ids_out.at[peer], dst_ref=ids_in.at[turn(m, peer, n)],
            send_sem=id_send.at[m], recv_sem=id_recv.at[turn(m, peer, n)],
            device_id={"dev": peer},
        )

    def id_arrival(m):
        peer = flip(me, turn(m, me, n, True), n)
        return pltpu.make_async_remote_copy(
            src_ref=ids_out.at[peer], dst_ref=ids_in.at[m],
            send_sem=id_send.at[m], recv_sem=id_recv.at[m],
            device_id={"dev": peer},
        )

    def row_copy(m):
        peer = flip(me, turn(m, me, n, True), n)
        return pltpu.make_async_remote_copy(
            src_ref=staging.at[m], dst_ref=rows.at[me],
            send_sem=row_send.at[m], recv_sem=row_recv.at[me],
            device_id={"dev": peer},
        )

    loop(1, n, lambda i: id_copy(n - i).start(), unroll=small)
    own_ids = pltpu.make_async_copy(ids_out.at[me], ids_in.at[0], own_sem)
    own_ids.start()

    tables_in.wait()
    tab32[pl.ds(zero_row, 8), :] = jnp.zeros((8, width), F32)
    step = 256

    def widen(i):
        for t in range(tabs):
            base = pl.multiple_of(i * step, step)
            tab32[pl.ds(t * vocab + base, step), :] = tab16[t, pl.ds(base, step), :].astype(F32)

    loop(0, vocab // step, widen)

    order_in.wait()
    inv_in.wait()
    loop(0, n, lambda g: place_targets(g, order, counts, inv, targets, expand), unroll=4)

    weight_in.wait()
    group = 8
    inner = group * mixes
    r, c = iota((inner, inner), 0), iota((inner, inner), 1)
    source = ((r // 8) % 2 * tabs + r % tabs) * mixes + 2 * (r // 16) + (r // 4) % 2
    reorder = jnp.where(c == source, 1.0, 0.0).astype(BF16)

    def order_weight(q):
        block = jnp.concatenate([weight[order[q * group + i]] for i in range(group)], axis=0)
        moved = jnp.dot(reorder, block, preferred_element_type=F32).astype(BF16)
        w_ref[:, pl.ds(pl.multiple_of(q * 16, 16), 16), :] = moved.reshape(mixes // 2, 16, -1)

    loop(0, slots // group, order_weight, unroll=4)

    compress_in.wait()
    across = f_ref.shape[1]
    spread = lax.dot_general(
        compress[...], expand[...].astype(BF16), (((1,), (1,)), ((), ())),
        preferred_element_type=F32,
    )
    sub, lane = iota((8, across), 0), iota((8, across), 1)
    same_half = (lane // tabs) % 2 == sub // 4
    for k in range(0, mixes, 2):
        for b in range(4):
            held = same_half & (sub % 4 == b)
            kept = [
                jnp.where(held, jnp.broadcast_to(spread[k + h:k + h + 1, :], (8, across)), 0.0)
                for h in range(2)
            ]
            mixer_ref[k * 8:k * 8 + 16, b * across:(b + 1) * across] = (
                jnp.concatenate(kept, axis=0).astype(BF16)
            )

    def pool(m, store):
        def row_block(i):
            at = pl.multiple_of(i * 16, 16)
            for r in range(16):
                total = None
                for p in range(pooling):
                    row = tab32[pl.ds(ids_in[m, p, at + r], 1), :]
                    total = row if total is None else total + row
                pooled[pl.ds(at + r, 1), :] = total

        loop(0, room // 16, row_block, unroll=True)
        store(pooled[...].astype(BF16))

    def store_own(value):
        rows[me] = value

    def serve(m):
        id_arrival(m).wait_recv()

        def store(value):
            staging[m] = value

        pool(m, store)
        row_copy(m).start()

    lax.fori_loop(1, n, lambda i, c: (serve(i), c)[1], 0, unroll=small)
    own_ids.wait()
    pool(0, store_own)
    if small:
        loop(0, n, lambda g: choose_rows(targets[g], choice, g), unroll=4)

    def select(i):
        q = flip(me // 2, i, n // 2)
        features = []
        for h in range(2):
            g = 2 * q + h
            at = g
            if not small:
                at = h
                choose_rows(targets[g], choice, h)
            packed = jnp.concatenate([rows[g], jnp.zeros((LANES - room, width), BF16)], axis=0)
            chosen = jnp.dot(choice[at], packed, preferred_element_type=F32)
            features.append(chosen.reshape(samples // 2, 8, width))
        f_ref[:, pl.ds(pl.multiple_of(q * 16, 16), 16), :] = (
            jnp.concatenate(features, axis=1).astype(BF16)
        )

    def arrival(m):
        peer = flip(me, m, n)
        pltpu.make_async_remote_copy(
            src_ref=staging.at[m], dst_ref=rows.at[peer],
            send_sem=row_send.at[m], recv_sem=row_recv.at[peer],
            device_id={"dev": peer},
        ).wait_recv()

    arrival(1)
    select(0)

    def collect(i):
        arrival(2 * i)
        arrival(2 * i + 1)
        select(i)

    loop(1, n // 2, collect)

    def finish(m):
        id_copy(m).wait_send()
        row_copy(m).wait_send()

    loop(1, n, finish, unroll=small)


def exchange(n, bags, lens, tables, inv, order, counts, compress, weight):
    tabs, vocab, width = tables.shape
    rows, slots = bags.shape
    most = lens.shape[0]
    pooling = rows // most
    samples, mixes, units = inv.shape[1], compress.shape[0], weight.shape[-1]
    room = PACK_ROOM
    assert tabs == PACK_GROUP and pooling == 4 and rows == LANES and n & (n - 1) == 0
    across = 2 * slots
    held = 3 * tables.size * 2 + 3 * weight.size * 2 + 3 * n * room * width * 4
    held += (samples * across * width + min(n, 16) * 4 * samples * LANES) * 2
    in_hbm = pl.BlockSpec(memory_space=pltpu.HBM)
    vmem = pl.BlockSpec(memory_space=pltpu.VMEM)
    operands = [
        pltpu.with_memory_space_constraint(x, pltpu.HBM)
        for x in (bags, lens, tables, inv, order, counts, compress, weight)
    ]
    return pl.pallas_call(
        functools.partial(exchange_kernel, n, most, room),
        out_shape=[
            jax.ShapeDtypeStruct((samples // 2, across, width), BF16),
            jax.ShapeDtypeStruct((mixes * 8, 4 * across), BF16),
            jax.ShapeDtypeStruct((mixes // 2, across, units), BF16),
        ],
        in_specs=[in_hbm] * 8,
        out_specs=[vmem] * 3,
        scratch_shapes=[
            pltpu.VMEM(bags.shape, I32),
            pltpu.VMEM(lens.shape, I32),
            pltpu.VMEM(tables.shape, BF16),
            pltpu.VMEM(inv.shape, I32),
            pltpu.SMEM(order.shape, I32),
            pltpu.SMEM(counts.shape, I32),
            pltpu.VMEM(compress.shape, BF16),
            pltpu.VMEM(weight.shape, BF16),
            pltpu.VMEM((tabs * vocab + 8, width), F32),
            pltpu.VMEM((slots, LANES), I32),
            pltpu.VMEM((slots, LANES), I32),
            pltpu.VMEM((n, pooling, LANES), I32),
            pltpu.SMEM((n, pooling, LANES), I32),
            pltpu.VMEM((room, width), F32),
            pltpu.VMEM((n, room, width), BF16),
            pltpu.VMEM((n, room, width), BF16),
            pltpu.VMEM((n, 2 * tabs, samples), I32),
            pltpu.VMEM((across, slots), F32),
            pltpu.VMEM((n if n <= 16 else 2, 4 * samples, LANES), BF16),
            pltpu.SemaphoreType.DMA((8,)),
            pltpu.SemaphoreType.DMA,
            pltpu.SemaphoreType.DMA((n,)),
            pltpu.SemaphoreType.DMA((n,)),
            pltpu.SemaphoreType.DMA((n,)),
            pltpu.SemaphoreType.DMA((n,)),
        ],
        compiler_params=pltpu.CompilerParams(
            collective_id=0, has_side_effects=True, vmem_limit_bytes=min(63 << 20, held + (6 << 20))
        ),
        name="exchange",
    )(*operands)


def interact_kernel(f_ref, mixer_ref, w_ref, bias_ref, out_ref, pairs, mixed):
    across, width = f_ref.shape[1:]
    mixes = mixer_ref.shape[0] // 8
    samples = out_ref.shape[0]
    sub, lane = iota((8, across), 0), iota((8, across), 1)
    first = sub < 4
    in_place = (lane // 4) % 2 == sub // 4
    mine = [sub % 4 == b for b in range(4)]

    def block(j):
        features = f_ref[pl.ds(j * 4, 4)].reshape(4 * across, width)
        products = lax.dot_general(
            mixed[j], features, (((1,), (1,)), ((), ())), preferred_element_type=F32
        )

        def of_mixture(k):
            parts = products[k * 8:k * 8 + 8, :]
            out = parts[:, :across]
            for b in range(1, 4):
                out = jnp.where(mine[b], parts[:, b * across:(b + 1) * across], out)
            return out

        for k in range(0, mixes, 2):
            even, odd = of_mixture(k), of_mixture(k + 1)
            stay, move = jnp.where(first, even, odd), jnp.where(first, odd, even)
            moved = jnp.where(first, pltpu.roll(move, 4, 1), pltpu.roll(move, across - 4, 1))
            pairs[pl.ds(pl.multiple_of(j * 8, 8), 8), k // 2 * across:(k // 2 + 1) * across] = (
                jnp.where(in_place, stay, moved)
            )

    def mix(i):
        features = [f_ref[pl.ds(i * 8 + h * 4, 4)].reshape(4 * across, width) for h in range(2)]
        both = jnp.dot(
            mixer_ref[...], jnp.concatenate(features, axis=1), preferred_element_type=F32
        ).astype(BF16)
        for h in range(2):
            mixed[2 * i + h] = both[:, h * width:(h + 1) * width]

    flat = samples <= LANES and across <= LANES
    loop(0, samples // 16, mix, unroll=flat)
    loop(0, samples // 8, block, unroll=flat)
    hidden = jnp.dot(
        pairs[...].astype(BF16), w_ref[...].reshape(mixes // 2 * across, -1),
        preferred_element_type=F32,
    ) + bias_ref[...]
    out_ref[...] = jnp.maximum(hidden, 0.0).astype(BF16)


def interact(features, mixer, weight, bias):
    pairs_of_samples, across, _ = features.shape
    samples, half_mixes, units = 2 * pairs_of_samples, weight.shape[0], weight.shape[2]
    held = (features.size + 2 * weight.size + mixer.size) * 2 + 6 * samples * half_mixes * across
    vmem = pl.BlockSpec(memory_space=pltpu.VMEM)
    return pl.pallas_call(
        interact_kernel,
        out_shape=jax.ShapeDtypeStruct((samples, units), BF16),
        in_specs=[vmem] * 4,
        out_specs=vmem,
        scratch_shapes=[
            pltpu.VMEM((samples, half_mixes * across), F32),
            pltpu.VMEM((samples // 8, mixer.shape[0], features.shape[2]), BF16),
        ],
        compiler_params=pltpu.CompilerParams(vmem_limit_bytes=min(63 << 20, held + (6 << 20))),
        name="interact",
    )(features, mixer, weight, bias)


def shards(
    n, tables, bag_rows, bag_lengths, row_counts, inverse, table_order, compress, top_weight, top_bias
):
    _, slots, most, pooling = bag_rows.shape
    mixes = compress.shape[0]
    features, mixer, weight = exchange(
        n, bag_rows[0].transpose(1, 2, 0).reshape(most * pooling, slots), bag_lengths[0].T, tables,
        inverse.T, table_order, row_counts[0], compress, top_weight.reshape(slots, mixes, -1),
    )
    return interact(features, mixer, weight, top_bias.reshape(1, -1))


def solution(mesh):
    return jax.shard_map(
        functools.partial(shards, mesh.shape["dev"]),
        mesh=mesh,
        in_specs=(
            P("dev", None, None),
            P(("rep", "dev"), None, None, None),
            P(("rep", "dev"), None, None),
            P(("rep", "dev"), None),
            P(("rep", "dev"), None),
            P(),
            P(),
            P(),
            P(),
        ),
        out_specs=P(("rep", "dev"), None),
        check_vma=False,
    )
```

```python
import functools

import jax
import jax.numpy as jnp
from jax import lax
from jax.experimental import pallas as pl
from jax.experimental.pallas import tpu as pltpu
from jax.sharding import PartitionSpec as P

F32 = jnp.float32
BF16 = jnp.bfloat16
I32 = jnp.int32
LANES = 128
PACK_GROUP, PACK_ROOM = 4, 80


def iota(shape, axis):
    return lax.broadcasted_iota(I32, shape, axis)


def flip(me, m, n):
    return me ^ m


def low(m, bit):
    return (m >> (bit.bit_length() - 1)) & 1


def wrap(m, n):
    return jnp.where(m >= n, m - (n - 1), m)


def turn(m, device, n, back=False):
    first = n - n // 4
    hops = low(device, 1) + low(device, 2) + (device >> 2)
    early = jnp.clip(2 * hops, 1, n - 1)
    late = wrap(device + n - first, n)
    at = m if back else wrap(m + n - first, n)
    moved = jnp.where(at == late, early, jnp.where(at == early, late, at))
    at = jnp.where(device == 0, at, moved)
    return wrap(at + first - 1, n) if back else at


def loop(start, stop, body, unroll=False):
    if unroll is True and stop - start <= 16:
        for i in range(start, stop):
            body(i)
        return

    def step(i, carry):
        body(i)
        return carry

    lax.fori_loop(start, stop, step, 0, unroll=unroll)


def pack_ids(q, most, vocab, zero_row, counts, xt, lt, ids_out):
    pooling = ids_out.shape[1]
    tabs = PACK_GROUP
    shape = (2 * pooling, LANES)
    sub, lane = iota(shape, 0), iota(shape, 1)
    high, p = sub >= pooling, sub % pooling
    first, second = 2 * q * tabs, (2 * q + 1) * tabs
    off_a, off_b = jnp.int32(0), jnp.int32(0)
    ids = jnp.full(shape, zero_row, I32)
    for t in range(tabs):
        count_a, count_b = counts[first + t], counts[second + t]
        unit = lane - jnp.where(high, off_b, off_a)
        at = jnp.clip(unit, 0, most - 1)
        rows = jnp.where(high, xt[pl.ds(second + t, 1), :], xt[pl.ds(first + t, 1), :])
        lengths = jnp.where(high, lt[pl.ds(second + t, 1), :], lt[pl.ds(first + t, 1), :])
        row = jnp.take_along_axis(rows, at * pooling + p, axis=1, mode="promise_in_bounds")
        length = jnp.take_along_axis(lengths, at, axis=1, mode="promise_in_bounds")
        used = (unit >= 0) & (unit < jnp.where(high, count_b, count_a)) & (p < length)
        ids = jnp.where(used, row + t * vocab, ids)
        off_a, off_b = off_a + count_a, off_b + count_b
    ids_out[2 * q] = ids[:pooling]
    ids_out[2 * q + 1] = ids[pooling:]


def place_targets(g, order, counts, inv, targets, expand):
    tabs = PACK_GROUP
    feature = iota((1, expand.shape[1]), 1)
    off = jnp.int32(0)
    for t in range(tabs):
        s = g * tabs + t
        count = counts[s]
        row = inv[pl.ds(order[s], 1), :]
        row = jnp.where(row < count, row + off, -1)
        targets[g, t:t + 1, :] = row
        targets[g, tabs + t:tabs + t + 1, :] = pltpu.roll(row, row.shape[1] - 4, 1)
        off = off + count
        hot = jnp.where(feature == order[s], 1.0, 0.0)
        expand[pl.ds(g * 2 * tabs + t, 1), :] = hot
        expand[pl.ds(g * 2 * tabs + tabs + t, 1), :] = hot


def choose_rows(target, choice, at):
    samples = target.shape[1]
    lane = iota((16, LANES), 1)
    pairs = [blk * 8 + b for blk in range(samples // 8) for b in range(4)]
    for i in range(0, len(pairs), 2):
        wide = jnp.concatenate(
            [jnp.broadcast_to(target[:, c:c + 1], (8, LANES)) for c in pairs[i:i + 2]], axis=0
        )
        choice[at, i * 8:i * 8 + 16, :] = jnp.where(wide == lane, 1.0, 0.0).astype(BF16)


def exchange_kernel(
    n, most, room,
    bags_hbm, lens_hbm, tables_hbm, inv_hbm, order_hbm, counts_hbm, compress_hbm, weight_hbm,
    f_ref, mixer_ref, w_ref,
    bags, lens, tab16, inv, order, counts, compress, weight,
    tab32, xt, lt, ids_out, ids_in, pooled, staging, rows, targets, expand, choice,
    local, own_sem, id_send, id_recv, row_send, row_recv,
):
    me = lax.axis_index("dev")
    tabs, vocab, width = tab16.shape
    slots, samples = inv.shape
    mixes = compress.shape[0]
    pooling = ids_out.shape[1]
    zero_row = tabs * vocab
    small = n <= 16

    barrier = pltpu.get_barrier_semaphore()
    loop(
        1, n,
        lambda i: pl.semaphore_signal(barrier, inc=1, device_id={"dev": flip(me, n - i, n)}),
        unroll=small,
    )

    copies = [
        pltpu.make_async_copy(src, dst, local.at[i])
        for i, (src, dst) in enumerate([
            (counts_hbm, counts), (bags_hbm, bags), (lens_hbm, lens), (order_hbm, order),
            (inv_hbm, inv), (compress_hbm, compress), (tables_hbm, tab16), (weight_hbm, weight),
        ])
    ]
    for copy in copies:
        copy.start()
    counts_in, bags_in, lens_in, order_in, inv_in, compress_in, tables_in, weight_in = copies

    bags_in.wait()
    xt[...] = bags[...].T
    lens_in.wait()
    lt[...] = jnp.concatenate(
        [lens[...], jnp.zeros((LANES - most, slots), I32)], axis=0
    ).T
    counts_in.wait()
    loop(
        0, n // 2, lambda q: pack_ids(q, most, vocab, zero_row, counts, xt, lt, ids_out),
        unroll=small,
    )
    pl.semaphore_wait(barrier, n - 1)

    def id_copy(m):
        peer = flip(me, m, n)
        return pltpu.make_async_remote_copy(
            src_ref=ids_out.at[peer], dst_ref=ids_in.at[turn(m, peer, n)],
            send_sem=id_send.at[m], recv_sem=id_recv.at[turn(m, peer, n)],
            device_id={"dev": peer},
        )

    def id_arrival(m):
        peer = flip(me, turn(m, me, n, True), n)
        return pltpu.make_async_remote_copy(
            src_ref=ids_out.at[peer], dst_ref=ids_in.at[m],
            send_sem=id_send.at[m], recv_sem=id_recv.at[m],
            device_id={"dev": peer},
        )

    def row_copy(m):
        peer = flip(me, turn(m, me, n, True), n)
        return pltpu.make_async_remote_copy(
            src_ref=staging.at[m], dst_ref=rows.at[me],
            send_sem=row_send.at[m], recv_sem=row_recv.at[me],
            device_id={"dev": peer},
        )

    loop(1, n, lambda i: id_copy(n - i).start(), unroll=small)
    own_ids = pltpu.make_async_copy(ids_out.at[me], ids_in.at[0], own_sem)
    own_ids.start()

    tables_in.wait()
    tab32[pl.ds(zero_row, 8), :] = jnp.zeros((8, width), F32)
    step = 256

    def widen(i):
        for t in range(tabs):
            base = pl.multiple_of(i * step, step)
            tab32[pl.ds(t * vocab + base, step), :] = tab16[t, pl.ds(base, step), :].astype(F32)

    loop(0, vocab // step, widen)

    order_in.wait()
    inv_in.wait()
    loop(0, n, lambda g: place_targets(g, order, counts, inv, targets, expand), unroll=4)

    weight_in.wait()
    group = 8
    inner = group * mixes
    r, c = iota((inner, inner), 0), iota((inner, inner), 1)
    source = ((r // 8) % 2 * tabs + r % tabs) * mixes + 2 * (r // 16) + (r // 4) % 2
    reorder = jnp.where(c == source, 1.0, 0.0).astype(BF16)

    def order_weight(q):
        block = jnp.concatenate([weight[order[q * group + i]] for i in range(group)], axis=0)
        moved = jnp.dot(reorder, block, preferred_element_type=F32).astype(BF16)
        w_ref[:, pl.ds(pl.multiple_of(q * 16, 16), 16), :] = moved.reshape(mixes // 2, 16, -1)

    loop(0, slots // group, order_weight, unroll=4)

    compress_in.wait()
    across = f_ref.shape[1]
    spread = lax.dot_general(
        compress[...], expand[...].astype(BF16), (((1,), (1,)), ((), ())),
        preferred_element_type=F32,
    )
    sub, lane = iota((8, across), 0), iota((8, across), 1)
    same_half = (lane // tabs) % 2 == sub // 4
    for k in range(0, mixes, 2):
        for b in range(4):
            held = same_half & (sub % 4 == b)
            kept = [
                jnp.where(held, jnp.broadcast_to(spread[k + h:k + h + 1, :], (8, across)), 0.0)
                for h in range(2)
            ]
            mixer_ref[k * 8:k * 8 + 16, b * across:(b + 1) * across] = (
                jnp.concatenate(kept, axis=0).astype(BF16)
            )

    def pool(m, store):
        def row_block(i):
            at = pl.multiple_of(i * 16, 16)
            for r in range(16):
                total = None
                for p in range(pooling):
                    row = tab32[pl.ds(ids_in[m, p, at + r], 1), :]
                    total = row if total is None else total + row
                pooled[pl.ds(at + r, 1), :] = total

        loop(0, room // 16, row_block, unroll=True)
        store(pooled[...].astype(BF16))

    def store_own(value):
        rows[me] = value

    def serve(m):
        id_arrival(m).wait_recv()

        def store(value):
            staging[m] = value

        pool(m, store)
        row_copy(m).start()

    lax.fori_loop(1, n, lambda i, c: (serve(i), c)[1], 0, unroll=small)
    own_ids.wait()
    pool(0, store_own)
    if small:
        loop(0, n, lambda g: choose_rows(targets[g], choice, g), unroll=4)

    def select(i):
        q = flip(me // 2, i, n // 2)
        features = []
        for h in range(2):
            g = 2 * q + h
            at = g
            if not small:
                at = h
                choose_rows(targets[g], choice, h)
            packed = jnp.concatenate([rows[g], jnp.zeros((LANES - room, width), BF16)], axis=0)
            chosen = jnp.dot(choice[at], packed, preferred_element_type=F32)
            features.append(chosen.reshape(samples // 2, 8, width))
        f_ref[:, pl.ds(pl.multiple_of(q * 16, 16), 16), :] = (
            jnp.concatenate(features, axis=1).astype(BF16)
        )

    def arrival(m):
        peer = flip(me, m, n)
        pltpu.make_async_remote_copy(
            src_ref=staging.at[m], dst_ref=rows.at[peer],
            send_sem=row_send.at[m], recv_sem=row_recv.at[peer],
            device_id={"dev": peer},
        ).wait_recv()

    arrival(1)
    select(0)

    def collect(i):
        arrival(2 * i)
        arrival(2 * i + 1)
        select(i)

    loop(1, n // 2, collect, unroll=small)

    def finish(m):
        id_copy(m).wait_send()
        row_copy(m).wait_send()

    loop(1, n, finish, unroll=small)


def exchange(n, bags, lens, tables, inv, order, counts, compress, weight):
    tabs, vocab, width = tables.shape
    rows, slots = bags.shape
    most = lens.shape[0]
    pooling = rows // most
    samples, mixes, units = inv.shape[1], compress.shape[0], weight.shape[-1]
    room = PACK_ROOM
    assert tabs == PACK_GROUP and pooling == 4 and rows == LANES and n & (n - 1) == 0
    across = 2 * slots
    held = 3 * tables.size * 2 + 3 * weight.size * 2 + 3 * n * room * width * 4
    held += (samples * across * width + min(n, 16) * 4 * samples * LANES) * 2
    in_hbm = pl.BlockSpec(memory_space=pltpu.HBM)
    vmem = pl.BlockSpec(memory_space=pltpu.VMEM)
    operands = [
        pltpu.with_memory_space_constraint(x, pltpu.HBM)
        for x in (bags, lens, tables, inv, order, counts, compress, weight)
    ]
    return pl.pallas_call(
        functools.partial(exchange_kernel, n, most, room),
        out_shape=[
            jax.ShapeDtypeStruct((samples // 2, across, width), BF16),
            jax.ShapeDtypeStruct((mixes * 8, 4 * across), BF16),
            jax.ShapeDtypeStruct((mixes // 2, across, units), BF16),
        ],
        in_specs=[in_hbm] * 8,
        out_specs=[vmem] * 3,
        scratch_shapes=[
            pltpu.VMEM(bags.shape, I32),
            pltpu.VMEM(lens.shape, I32),
            pltpu.VMEM(tables.shape, BF16),
            pltpu.VMEM(inv.shape, I32),
            pltpu.SMEM(order.shape, I32),
            pltpu.SMEM(counts.shape, I32),
            pltpu.VMEM(compress.shape, BF16),
            pltpu.VMEM(weight.shape, BF16),
            pltpu.VMEM((tabs * vocab + 8, width), F32),
            pltpu.VMEM((slots, LANES), I32),
            pltpu.VMEM((slots, LANES), I32),
            pltpu.VMEM((n, pooling, LANES), I32),
            pltpu.SMEM((n, pooling, LANES), I32),
            pltpu.VMEM((room, width), F32),
            pltpu.VMEM((n, room, width), BF16),
            pltpu.VMEM((n, room, width), BF16),
            pltpu.VMEM((n, 2 * tabs, samples), I32),
            pltpu.VMEM((across, slots), F32),
            pltpu.VMEM((n if n <= 16 else 2, 4 * samples, LANES), BF16),
            pltpu.SemaphoreType.DMA((8,)),
            pltpu.SemaphoreType.DMA,
            pltpu.SemaphoreType.DMA((n,)),
            pltpu.SemaphoreType.DMA((n,)),
            pltpu.SemaphoreType.DMA((n,)),
            pltpu.SemaphoreType.DMA((n,)),
        ],
        compiler_params=pltpu.CompilerParams(
            collective_id=0, has_side_effects=True, vmem_limit_bytes=min(63 << 20, held + (6 << 20))
        ),
        name="exchange",
    )(*operands)


def interact_kernel(f_ref, mixer_ref, w_ref, bias_ref, out_ref, pairs, mixed):
    across, width = f_ref.shape[1:]
    mixes = mixer_ref.shape[0] // 8
    samples = out_ref.shape[0]
    sub, lane = iota((8, across), 0), iota((8, across), 1)
    first = sub < 4
    in_place = (lane // 4) % 2 == sub // 4
    mine = [sub % 4 == b for b in range(4)]

    def block(j):
        features = f_ref[pl.ds(j * 4, 4)].reshape(4 * across, width)
        products = lax.dot_general(
            mixed[j], features, (((1,), (1,)), ((), ())), preferred_element_type=F32
        )

        def of_mixture(k):
            parts = products[k * 8:k * 8 + 8, :]
            out = parts[:, :across]
            for b in range(1, 4):
                out = jnp.where(mine[b], parts[:, b * across:(b + 1) * across], out)
            return out

        for k in range(0, mixes, 2):
            even, odd = of_mixture(k), of_mixture(k + 1)
            stay, move = jnp.where(first, even, odd), jnp.where(first, odd, even)
            moved = jnp.where(first, pltpu.roll(move, 4, 1), pltpu.roll(move, across - 4, 1))
            pairs[pl.ds(pl.multiple_of(j * 8, 8), 8), k // 2 * across:(k // 2 + 1) * across] = (
                jnp.where(in_place, stay, moved)
            )

    def mix(i):
        features = [f_ref[pl.ds(i * 8 + h * 4, 4)].reshape(4 * across, width) for h in range(2)]
        both = jnp.dot(
            mixer_ref[...], jnp.concatenate(features, axis=1), preferred_element_type=F32
        ).astype(BF16)
        for h in range(2):
            mixed[2 * i + h] = both[:, h * width:(h + 1) * width]

    flat = samples <= LANES and across <= LANES
    loop(0, samples // 16, mix, unroll=flat)
    loop(0, samples // 8, block, unroll=flat)
    hidden = jnp.dot(
        pairs[...].astype(BF16), w_ref[...].reshape(mixes // 2 * across, -1),
        preferred_element_type=F32,
    ) + bias_ref[...]
    out_ref[...] = jnp.maximum(hidden, 0.0).astype(BF16)


def interact(features, mixer, weight, bias):
    pairs_of_samples, across, _ = features.shape
    samples, half_mixes, units = 2 * pairs_of_samples, weight.shape[0], weight.shape[2]
    held = (features.size + 2 * weight.size + mixer.size) * 2 + 6 * samples * half_mixes * across
    vmem = pl.BlockSpec(memory_space=pltpu.VMEM)
    return pl.pallas_call(
        interact_kernel,
        out_shape=jax.ShapeDtypeStruct((samples, units), BF16),
        in_specs=[vmem] * 4,
        out_specs=vmem,
        scratch_shapes=[
            pltpu.VMEM((samples, half_mixes * across), F32),
            pltpu.VMEM((samples // 8, mixer.shape[0], features.shape[2]), BF16),
        ],
        compiler_params=pltpu.CompilerParams(vmem_limit_bytes=min(63 << 20, held + (6 << 20))),
        name="interact",
    )(features, mixer, weight, bias)


def shards(
    n, tables, bag_rows, bag_lengths, row_counts, inverse, table_order, compress, top_weight, top_bias
):
    _, slots, most, pooling = bag_rows.shape
    mixes = compress.shape[0]
    features, mixer, weight = exchange(
        n, bag_rows[0].transpose(1, 2, 0).reshape(most * pooling, slots), bag_lengths[0].T, tables,
        inverse.T, table_order, row_counts[0], compress, top_weight.reshape(slots, mixes, -1),
    )
    return interact(features, mixer, weight, top_bias.reshape(1, -1))


def solution(mesh):
    return jax.shard_map(
        functools.partial(shards, mesh.shape["dev"]),
        mesh=mesh,
        in_specs=(
            P("dev", None, None),
            P(("rep", "dev"), None, None, None),
            P(("rep", "dev"), None, None),
            P(("rep", "dev"), None),
            P(("rep", "dev"), None),
            P(),
            P(),
            P(),
            P(),
        ),
        out_specs=P(("rep", "dev"), None),
        check_vma=False,
    )
```

```python
import functools

import jax
import jax.numpy as jnp
from jax import lax
from jax.experimental import pallas as pl
from jax.experimental.pallas import tpu as pltpu
from jax.sharding import PartitionSpec as P

F32 = jnp.float32
BF16 = jnp.bfloat16
I32 = jnp.int32
LANES = 128
PACK_GROUP, PACK_ROOM = 4, 80


def iota(shape, axis):
    return lax.broadcasted_iota(I32, shape, axis)


def flip(me, m, n):
    return me ^ m


def low(m, bit):
    return (m >> (bit.bit_length() - 1)) & 1


def wrap(m, n):
    return jnp.where(m >= n, m - (n - 1), m)


def turn(m, device, n, back=False):
    first = n - n // 4
    hops = low(device, 1) + low(device, 2) + (device >> 2)
    early = jnp.clip(2 * hops, 1, n - 1)
    late = wrap(device + n - first, n)
    at = m if back else wrap(m + n - first, n)
    moved = jnp.where(at == late, early, jnp.where(at == early, late, at))
    at = jnp.where(device == 0, at, moved)
    return wrap(at + first - 1, n) if back else at


def loop(start, stop, body, unroll=False):
    if unroll is True and stop - start <= 16:
        for i in range(start, stop):
            body(i)
        return

    def step(i, carry):
        body(i)
        return carry

    lax.fori_loop(start, stop, step, 0, unroll=unroll)


def pack_ids(q, most, vocab, zero_row, counts, xt, lt, ids_out):
    pooling = ids_out.shape[1]
    tabs = PACK_GROUP
    shape = (2 * pooling, LANES)
    sub, lane = iota(shape, 0), iota(shape, 1)
    high, p = sub >= pooling, sub % pooling
    first, second = 2 * q * tabs, (2 * q + 1) * tabs
    off_a, off_b = jnp.int32(0), jnp.int32(0)
    ids = jnp.full(shape, zero_row, I32)
    for t in range(tabs):
        count_a, count_b = counts[first + t], counts[second + t]
        unit = lane - jnp.where(high, off_b, off_a)
        at = jnp.clip(unit, 0, most - 1)
        rows = jnp.where(high, xt[pl.ds(second + t, 1), :], xt[pl.ds(first + t, 1), :])
        lengths = jnp.where(high, lt[pl.ds(second + t, 1), :], lt[pl.ds(first + t, 1), :])
        row = jnp.take_along_axis(rows, at * pooling + p, axis=1, mode="promise_in_bounds")
        length = jnp.take_along_axis(lengths, at, axis=1, mode="promise_in_bounds")
        used = (unit >= 0) & (unit < jnp.where(high, count_b, count_a)) & (p < length)
        ids = jnp.where(used, row + t * vocab, ids)
        off_a, off_b = off_a + count_a, off_b + count_b
    ids_out[2 * q] = ids[:pooling]
    ids_out[2 * q + 1] = ids[pooling:]


def place_targets(g, order, counts, inv, targets, expand):
    tabs = PACK_GROUP
    feature = iota((1, expand.shape[1]), 1)
    off = jnp.int32(0)
    for t in range(tabs):
        s = g * tabs + t
        count = counts[s]
        row = inv[pl.ds(order[s], 1), :]
        row = jnp.where(row < count, row + off, -1)
        targets[g, t:t + 1, :] = row
        targets[g, tabs + t:tabs + t + 1, :] = pltpu.roll(row, row.shape[1] - 4, 1)
        off = off + count
        hot = jnp.where(feature == order[s], 1.0, 0.0)
        expand[pl.ds(g * 2 * tabs + t, 1), :] = hot
        expand[pl.ds(g * 2 * tabs + tabs + t, 1), :] = hot


def choose_rows(target, choice, at):
    samples = target.shape[1]
    lane = iota((16, LANES), 1)
    pairs = [blk * 8 + b for blk in range(samples // 8) for b in range(4)]
    for i in range(0, len(pairs), 2):
        wide = jnp.concatenate(
            [jnp.broadcast_to(target[:, c:c + 1], (8, LANES)) for c in pairs[i:i + 2]], axis=0
        )
        choice[at, i * 8:i * 8 + 16, :] = jnp.where(wide == lane, 1.0, 0.0).astype(BF16)


def exchange_kernel(
    n, most, room,
    bags_hbm, lens_hbm, tables_hbm, inv_hbm, order_hbm, counts_hbm, compress_hbm, weight_hbm,
    f_ref, mixer_ref, w_ref,
    bags, lens, tab16, inv, order, counts, compress, weight,
    tab32, xt, lt, ids_out, ids_in, pooled, staging, rows, targets, expand, choice,
    local, own_sem, id_send, id_recv, row_send, row_recv,
):
    me = lax.axis_index("dev")
    tabs, vocab, width = tab16.shape
    slots, samples = inv.shape
    mixes = compress.shape[0]
    pooling = ids_out.shape[1]
    zero_row = tabs * vocab
    small = n <= 16

    barrier = pltpu.get_barrier_semaphore()
    loop(
        1, n,
        lambda i: pl.semaphore_signal(barrier, inc=1, device_id={"dev": flip(me, n - i, n)}),
        unroll=small,
    )

    copies = [
        pltpu.make_async_copy(src, dst, local.at[i])
        for i, (src, dst) in enumerate([
            (counts_hbm, counts), (bags_hbm, bags), (lens_hbm, lens), (order_hbm, order),
            (inv_hbm, inv), (compress_hbm, compress), (tables_hbm, tab16), (weight_hbm, weight),
        ])
    ]
    for copy in copies:
        copy.start()
    counts_in, bags_in, lens_in, order_in, inv_in, compress_in, tables_in, weight_in = copies

    bags_in.wait()
    xt[...] = bags[...].T
    lens_in.wait()
    lt[...] = jnp.concatenate(
        [lens[...], jnp.zeros((LANES - most, slots), I32)], axis=0
    ).T
    counts_in.wait()
    loop(
        0, n // 2, lambda q: pack_ids(q, most, vocab, zero_row, counts, xt, lt, ids_out),
        unroll=small,
    )
    pl.semaphore_wait(barrier, n - 1)

    def id_copy(m):
        peer = flip(me, m, n)
        return pltpu.make_async_remote_copy(
            src_ref=ids_out.at[peer], dst_ref=ids_in.at[turn(m, peer, n)],
            send_sem=id_send.at[m], recv_sem=id_recv.at[turn(m, peer, n)],
            device_id={"dev": peer},
        )

    def id_arrival(m):
        peer = flip(me, turn(m, me, n, True), n)
        return pltpu.make_async_remote_copy(
            src_ref=ids_out.at[peer], dst_ref=ids_in.at[m],
            send_sem=id_send.at[m], recv_sem=id_recv.at[m],
            device_id={"dev": peer},
        )

    def row_copy(m):
        peer = flip(me, turn(m, me, n, True), n)
        return pltpu.make_async_remote_copy(
            src_ref=staging.at[m], dst_ref=rows.at[me],
            send_sem=row_send.at[m], recv_sem=row_recv.at[me],
            device_id={"dev": peer},
        )

    loop(1, n, lambda i: id_copy(n - i).start(), unroll=small)
    own_ids = pltpu.make_async_copy(ids_out.at[me], ids_in.at[0], own_sem)
    own_ids.start()

    tables_in.wait()
    tab32[pl.ds(zero_row, 8), :] = jnp.zeros((8, width), F32)
    step = 256

    def widen(i):
        for t in range(tabs):
            base = pl.multiple_of(i * step, step)
            tab32[pl.ds(t * vocab + base, step), :] = tab16[t, pl.ds(base, step), :].astype(F32)

    loop(0, vocab // step, widen)

    order_in.wait()
    inv_in.wait()
    loop(0, n, lambda g: place_targets(g, order, counts, inv, targets, expand), unroll=4)

    weight_in.wait()
    group = 8
    inner = group * mixes
    r, c = iota((inner, inner), 0), iota((inner, inner), 1)
    source = ((r // 8) % 2 * tabs + r % tabs) * mixes + 2 * (r // 16) + (r // 4) % 2
    reorder = jnp.where(c == source, 1.0, 0.0).astype(BF16)

    def order_weight(q):
        block = jnp.concatenate([weight[order[q * group + i]] for i in range(group)], axis=0)
        moved = jnp.dot(reorder, block, preferred_element_type=F32).astype(BF16)
        w_ref[:, pl.ds(pl.multiple_of(q * 16, 16), 16), :] = moved.reshape(mixes // 2, 16, -1)

    loop(0, slots // group, order_weight, unroll=4)

    compress_in.wait()
    across = f_ref.shape[1]
    spread = lax.dot_general(
        compress[...], expand[...].astype(BF16), (((1,), (1,)), ((), ())),
        preferred_element_type=F32,
    )
    sub, lane = iota((8, across), 0), iota((8, across), 1)
    same_half = (lane // tabs) % 2 == sub // 4
    for k in range(0, mixes, 2):
        for b in range(4):
            held = same_half & (sub % 4 == b)
            kept = [
                jnp.where(held, jnp.broadcast_to(spread[k + h:k + h + 1, :], (8, across)), 0.0)
                for h in range(2)
            ]
            mixer_ref[k * 8:k * 8 + 16, b * across:(b + 1) * across] = (
                jnp.concatenate(kept, axis=0).astype(BF16)
            )

    def pool(m, store):
        def row_block(i):
            at = pl.multiple_of(i * 16, 16)
            for r in range(16):
                total = None
                for p in range(pooling):
                    row = tab32[pl.ds(ids_in[m, p, at + r], 1), :]
                    total = row if total is None else total + row
                pooled[pl.ds(at + r, 1), :] = total

        loop(0, room // 16, row_block, unroll=True)
        store(pooled[...].astype(BF16))

    def store_own(value):
        rows[me] = value

    def serve(m):
        id_arrival(m).wait_recv()

        def store(value):
            staging[m] = value

        pool(m, store)
        row_copy(m).start()

    lax.fori_loop(1, n, lambda i, c: (serve(i), c)[1], 0, unroll=small)
    own_ids.wait()
    pool(0, store_own)
    if small:
        loop(0, n, lambda g: choose_rows(targets[g], choice, g), unroll=4)

    def select(i):
        q = flip(me // 2, i, n // 2)
        features = []
        for h in range(2):
            g = 2 * q + h
            at = g
            if not small:
                at = h
                choose_rows(targets[g], choice, h)
            packed = jnp.concatenate([rows[g], jnp.zeros((LANES - room, width), BF16)], axis=0)
            chosen = jnp.dot(choice[at], packed, preferred_element_type=F32)
            features.append(chosen.reshape(samples // 2, 8, width))
        f_ref[:, pl.ds(pl.multiple_of(q * 16, 16), 16), :] = (
            jnp.concatenate(features, axis=1).astype(BF16)
        )

    def arrival(m):
        peer = flip(me, m, n)
        pltpu.make_async_remote_copy(
            src_ref=staging.at[m], dst_ref=rows.at[peer],
            send_sem=row_send.at[m], recv_sem=row_recv.at[peer],
            device_id={"dev": peer},
        ).wait_recv()

    loop(1, n, lambda m: id_copy(m).wait_send(), unroll=small)
    arrival(1)
    select(0)

    def collect(i):
        arrival(2 * i)
        arrival(2 * i + 1)
        select(i)

    loop(1, n // 2 - 1, collect, unroll=small)
    loop(1, n, lambda m: row_copy(m).wait_send(), unroll=small)
    collect(n // 2 - 1)


def exchange(n, bags, lens, tables, inv, order, counts, compress, weight):
    tabs, vocab, width = tables.shape
    rows, slots = bags.shape
    most = lens.shape[0]
    pooling = rows // most
    samples, mixes, units = inv.shape[1], compress.shape[0], weight.shape[-1]
    room = PACK_ROOM
    assert tabs == PACK_GROUP and pooling == 4 and rows == LANES and n & (n - 1) == 0
    across = 2 * slots
    held = 3 * tables.size * 2 + 3 * weight.size * 2 + 3 * n * room * width * 4
    held += (samples * across * width + min(n, 16) * 4 * samples * LANES) * 2
    in_hbm = pl.BlockSpec(memory_space=pltpu.HBM)
    vmem = pl.BlockSpec(memory_space=pltpu.VMEM)
    operands = [
        pltpu.with_memory_space_constraint(x, pltpu.HBM)
        for x in (bags, lens, tables, inv, order, counts, compress, weight)
    ]
    return pl.pallas_call(
        functools.partial(exchange_kernel, n, most, room),
        out_shape=[
            jax.ShapeDtypeStruct((samples // 2, across, width), BF16),
            jax.ShapeDtypeStruct((mixes * 8, 4 * across), BF16),
            jax.ShapeDtypeStruct((mixes // 2, across, units), BF16),
        ],
        in_specs=[in_hbm] * 8,
        out_specs=[vmem] * 3,
        scratch_shapes=[
            pltpu.VMEM(bags.shape, I32),
            pltpu.VMEM(lens.shape, I32),
            pltpu.VMEM(tables.shape, BF16),
            pltpu.VMEM(inv.shape, I32),
            pltpu.SMEM(order.shape, I32),
            pltpu.SMEM(counts.shape, I32),
            pltpu.VMEM(compress.shape, BF16),
            pltpu.VMEM(weight.shape, BF16),
            pltpu.VMEM((tabs * vocab + 8, width), F32),
            pltpu.VMEM((slots, LANES), I32),
            pltpu.VMEM((slots, LANES), I32),
            pltpu.VMEM((n, pooling, LANES), I32),
            pltpu.SMEM((n, pooling, LANES), I32),
            pltpu.VMEM((room, width), F32),
            pltpu.VMEM((n, room, width), BF16),
            pltpu.VMEM((n, room, width), BF16),
            pltpu.VMEM((n, 2 * tabs, samples), I32),
            pltpu.VMEM((across, slots), F32),
            pltpu.VMEM((n if n <= 16 else 2, 4 * samples, LANES), BF16),
            pltpu.SemaphoreType.DMA((8,)),
            pltpu.SemaphoreType.DMA,
            pltpu.SemaphoreType.DMA((n,)),
            pltpu.SemaphoreType.DMA((n,)),
            pltpu.SemaphoreType.DMA((n,)),
            pltpu.SemaphoreType.DMA((n,)),
        ],
        compiler_params=pltpu.CompilerParams(
            collective_id=0, has_side_effects=True, vmem_limit_bytes=min(63 << 20, held + (6 << 20))
        ),
        name="exchange",
    )(*operands)


def interact_kernel(f_ref, mixer_ref, w_ref, bias_ref, out_ref, pairs, mixed):
    across, width = f_ref.shape[1:]
    mixes = mixer_ref.shape[0] // 8
    samples = out_ref.shape[0]
    sub, lane = iota((8, across), 0), iota((8, across), 1)
    first = sub < 4
    in_place = (lane // 4) % 2 == sub // 4
    mine = [sub % 4 == b for b in range(4)]

    def block(j):
        features = f_ref[pl.ds(j * 4, 4)].reshape(4 * across, width)
        products = lax.dot_general(
            mixed[j], features, (((1,), (1,)), ((), ())), preferred_element_type=F32
        )

        def of_mixture(k):
            parts = products[k * 8:k * 8 + 8, :]
            out = parts[:, :across]
            for b in range(1, 4):
                out = jnp.where(mine[b], parts[:, b * across:(b + 1) * across], out)
            return out

        for k in range(0, mixes, 2):
            even, odd = of_mixture(k), of_mixture(k + 1)
            stay, move = jnp.where(first, even, odd), jnp.where(first, odd, even)
            moved = jnp.where(first, pltpu.roll(move, 4, 1), pltpu.roll(move, across - 4, 1))
            pairs[pl.ds(pl.multiple_of(j * 8, 8), 8), k // 2 * across:(k // 2 + 1) * across] = (
                jnp.where(in_place, stay, moved)
            )

    def mix(i):
        features = [f_ref[pl.ds(i * 8 + h * 4, 4)].reshape(4 * across, width) for h in range(2)]
        both = jnp.dot(
            mixer_ref[...], jnp.concatenate(features, axis=1), preferred_element_type=F32
        ).astype(BF16)
        for h in range(2):
            mixed[2 * i + h] = both[:, h * width:(h + 1) * width]

    flat = samples <= LANES and across <= LANES
    loop(0, samples // 16, mix, unroll=flat)
    loop(0, samples // 8, block, unroll=flat)
    hidden = jnp.dot(
        pairs[...].astype(BF16), w_ref[...].reshape(mixes // 2 * across, -1),
        preferred_element_type=F32,
    ) + bias_ref[...]
    out_ref[...] = jnp.maximum(hidden, 0.0).astype(BF16)


def interact(features, mixer, weight, bias):
    pairs_of_samples, across, _ = features.shape
    samples, half_mixes, units = 2 * pairs_of_samples, weight.shape[0], weight.shape[2]
    held = (features.size + 2 * weight.size + mixer.size) * 2 + 6 * samples * half_mixes * across
    vmem = pl.BlockSpec(memory_space=pltpu.VMEM)
    return pl.pallas_call(
        interact_kernel,
        out_shape=jax.ShapeDtypeStruct((samples, units), BF16),
        in_specs=[vmem] * 4,
        out_specs=vmem,
        scratch_shapes=[
            pltpu.VMEM((samples, half_mixes * across), F32),
            pltpu.VMEM((samples // 8, mixer.shape[0], features.shape[2]), BF16),
        ],
        compiler_params=pltpu.CompilerParams(vmem_limit_bytes=min(63 << 20, held + (6 << 20))),
        name="interact",
    )(features, mixer, weight, bias)


def shards(
    n, tables, bag_rows, bag_lengths, row_counts, inverse, table_order, compress, top_weight, top_bias
):
    _, slots, most, pooling = bag_rows.shape
    mixes = compress.shape[0]
    features, mixer, weight = exchange(
        n, bag_rows[0].transpose(1, 2, 0).reshape(most * pooling, slots), bag_lengths[0].T, tables,
        inverse.T, table_order, row_counts[0], compress, top_weight.reshape(slots, mixes, -1),
    )
    return interact(features, mixer, weight, top_bias.reshape(1, -1))


def solution(mesh):
    return jax.shard_map(
        functools.partial(shards, mesh.shape["dev"]),
        mesh=mesh,
        in_specs=(
            P("dev", None, None),
            P(("rep", "dev"), None, None, None),
            P(("rep", "dev"), None, None),
            P(("rep", "dev"), None),
            P(("rep", "dev"), None),
            P(),
            P(),
            P(),
            P(),
        ),
        out_specs=P(("rep", "dev"), None),
        check_vma=False,
    )
```
